32 devices in a mesh: dp: 8 (over z, x), owner: 4 (over y, core).
Axes of the slice: x: 2, y: 2, z: 4, core: 2. Of those that a mesh axis runs over, the one named last changes fastest.
Arguments:
- gradients: float32 [8, 1024, 7168], P(None, 'dp', 'owner'), may hold values from -6 to 6
- rows_live: int32 [8], replicated, may hold values from 256 to 1024
Outputs:
- updates: bfloat16 [8, 1024, 7168], P(None, 'dp', 'owner')
The draws below stay inside these ranges and needn't reach their ends.
All inputs are finite; a program needn't handle non-finite values.
Results may differ from the reference program's by a relative error of at most 0.015.
Values may be sent and summed in bfloat16 or wider, within the bound.
A program may use at most 64 MiB of HBM per device.

```python
import math
import jax
import jax.numpy as jnp
from jax import lax

D = 7168
FF_WIN = 1024
MATRICES = 8
N_OWNER = 4


def with_ends(values, stream_key, smallest, top_value):
    shape = values.shape
    spot = [jax.random.randint(jax.random.fold_in(stream_key, axis), (), 0, shape[axis]) for axis in range(len(shape))]
    values = values.at[tuple(spot)].set(smallest)
    longest = shape.index(max(shape))
    spot[longest] = (spot[longest] + 1) % shape[longest]
    return values.at[tuple(spot)].set(top_value)


def shard_levels(key, dims, cuts, smallest, top_value):
    factor_of, own = 1.0, jax.random.fold_in(key, 6)
    for dim, parts in cuts:
        steps = jnp.exp(jax.random.uniform(jax.random.fold_in(own, dim), (parts,), jnp.float32, smallest / len(cuts), top_value / len(cuts)))
        factor_of = factor_of * jnp.repeat(steps, dims[dim] // parts).reshape([-1 if axis == dim else 1 for axis in range(len(dims))])
    return factor_of


def scatter_about(stream_key, shape, deviation, bound, pieces=(), kind=jnp.bfloat16):
    array = deviation * jax.random.normal(stream_key, shape, jnp.float32)
    if pieces:
        array = array * shard_levels(stream_key, shape, pieces, -0.22, 0.18)
    return jnp.clip(array, -bound, bound).astype(kind)


def setup_inputs(seed: int = 0) -> dict:
    arg_keys = jax.random.split(jax.random.key(seed), 3)
    gradients = scatter_about(arg_keys[0], (MATRICES, FF_WIN, D), 1.0, 6.0, ((1, 8), (2, 4)), jnp.float32)
    rows_live = with_ends(jax.random.randint(arg_keys[1], (MATRICES,), FF_WIN // 4, FF_WIN + 1), jax.random.fold_in(arg_keys[1], 1), FF_WIN // 4, FF_WIN).astype(jnp.int32)
    return dict(gradients=gradients, rows_live=rows_live)


def one_matrix(packed):
    gradient, live_count = packed
    narrow = gradient.astype(jnp.bfloat16)
    live_mask = jnp.arange(FF_WIN, dtype=jnp.int32)[:, None] < live_count
    narrow = jnp.where(live_mask, narrow, jnp.zeros_like(narrow))
    width = D // N_OWNER
    blocks = narrow.reshape(FF_WIN, N_OWNER, width).transpose(1, 0, 2)

    def add_block(total, block):
        term = jnp.dot(block, block.T, preferred_element_type=jnp.float32)
        rounded = lax.optimization_barrier(term.astype(jnp.bfloat16))
        return (total + rounded.astype(jnp.float32), None)
    gram, unused = lax.scan(add_block, jnp.zeros((FF_WIN, FF_WIN), jnp.float32), blocks)
    scale_sq = 2.0 * jnp.trace(gram) / live_count.astype(jnp.float32)
    inverse = 1.0 / jnp.sqrt(scale_sq)
    normed_gram = (gram / scale_sq).astype(jnp.bfloat16)
    once = jnp.dot(normed_gram, narrow, preferred_element_type=jnp.float32) * inverse
    twice = jnp.dot(normed_gram, once.astype(jnp.bfloat16), preferred_element_type=jnp.float32)
    result = 3.4445 * narrow.astype(jnp.float32) * inverse - 4.775 * once + 2.0315 * twice
    return (result * (0.2 * math.sqrt(D))).astype(jnp.bfloat16)

def reference(gradients, rows_live):
    return lax.map(one_matrix, (gradients, rows_live))
```

```python
import functools
import math

import jax
import jax.numpy as jnp
from jax import lax
from jax.experimental import pallas as pl
from jax.experimental.pallas import tpu as pltpu
from jax.sharding import PartitionSpec as P

MESH = pl.DeviceIdType.MESH
NT = (((1,), (1,)), ((), ()))
NN = (((1,), (0,)), ((), ()))


def flip(index, bits, count):
    out, bit = 0, 1
    while bit < count:
        out = out + bit * (((index // bit) % 2 + (bits // bit) % 2) % 2)
        bit *= 2
    return out


def kernel(
    n, owners, width_all, live_ref, grad_ref, out_ref,
    stage, send, rows, gram, normed, upd, part, got,
    load_sem, send_sem, recv_sem, psend_sem, precv_sem, usend_sem, urecv_sem, own_sem,
):
    d = lax.axis_index("dp")
    o = lax.axis_index("owner")
    size, width = stage.shape[1], stage.shape[2]
    hidden = rows.shape[0]
    strip = max(size, min(128, hidden))
    strips = hidden // strip
    per = strip // size
    levels = owners.bit_length() - 1

    def far_first(j):
        return 1 + (j + n // 2 - 1) % (n - 1)

    def load(slot):
        return pltpu.make_async_copy(grad_ref.at[flip(d, slot, n)], stage.at[slot], load_sem.at[slot])

    def forward(slot):
        return pltpu.make_async_remote_copy(
            src_ref=send.at[slot],
            dst_ref=rows.at[pl.ds(pl.multiple_of(slot * size, size), size)],
            send_sem=send_sem.at[slot],
            recv_sem=recv_sem.at[slot],
            device_id={"dp": flip(d, slot, n)},
            device_id_type=MESH,
        )

    def back(slot):
        return pltpu.make_async_remote_copy(
            src_ref=upd.at[pl.ds(pl.multiple_of(slot * size, size), size)],
            dst_ref=out_ref.at[d],
            send_sem=usend_sem.at[slot],
            recv_sem=urecv_sem.at[slot],
            device_id={"dp": flip(d, slot, n)},
            device_id_type=MESH,
        )

    def back_arrival(slot):
        return pltpu.make_async_remote_copy(
            src_ref=upd.at[pl.ds(pl.multiple_of(slot * size, size), size)],
            dst_ref=out_ref.at[flip(d, slot, n)],
            send_sem=usend_sem.at[slot],
            recv_sem=urecv_sem.at[slot],
            device_id={"dp": flip(d, slot, n)},
            device_id_type=MESH,
        )

    def share(level, s):
        cols = (s + 1) * strip
        return pltpu.make_async_remote_copy(
            src_ref=part.at[level, s, :, pl.ds(0, cols)],
            dst_ref=got.at[level, s, :, pl.ds(0, cols)],
            send_sem=psend_sem.at[level, s],
            recv_sem=precv_sem.at[level, s],
            device_id={"owner": flip(o, 2**level, owners)},
            device_id_type=MESH,
        )

    @pl.loop(0, n - 1)
    def _(j):
        load(far_first(j)).start()

    load(0).start()

    barrier = pltpu.get_barrier_semaphore()

    @pl.loop(1, n)
    def _(k):
        pl.semaphore_signal(barrier, inc=1, device_id={"dp": flip(d, k, n)}, device_id_type=MESH)

    for level in range(levels):
        pl.semaphore_signal(
            barrier, inc=1, device_id={"owner": flip(o, 2**level, owners)}, device_id_type=MESH
        )
    pl.semaphore_wait(barrier, n - 1 + levels)

    row_index = d * size + lax.broadcasted_iota(jnp.int32, (size, width), 0)

    def narrow(slot):
        load(slot).wait()
        live = live_ref[flip(d, slot, n)]
        return jnp.where(row_index < live, stage[slot], 0.0).astype(jnp.bfloat16)

    @pl.loop(0, n - 1)
    def _(j):
        slot = far_first(j)
        send[slot] = narrow(slot)
        forward(slot).start()

    rows[pl.ds(0, size), :] = narrow(0)

    eye = (
        lax.broadcasted_iota(jnp.int32, (strip, strip), 0)
        == lax.broadcasted_iota(jnp.int32, (strip, strip), 1)
    )
    trace = jnp.zeros((1, 1), jnp.float32)

    def settle(s, trace):
        at = s * strip
        cols = at + strip
        share(levels - 1, s).wait_recv()
        total = (
            part[levels - 1, s, :, 0:cols].astype(jnp.float32)
            + got[levels - 1, s, :, 0:cols].astype(jnp.float32)
        )
        gram[at:cols, 0:cols] = total
        for j in range(s):
            gram[j * strip : (j + 1) * strip, at:cols] = total[:, j * strip : (j + 1) * strip].T
        own = jnp.where(eye, total[:, at:cols], 0.0)
        return trace + jnp.sum(own, keepdims=True)

    for s in range(strips):
        cols = (s + 1) * strip
        if s == 0:
            @pl.loop(1, per)
            def _(k):
                forward(k).wait_recv()
        else:
            @pl.loop(s * per, (s + 1) * per)
            def _(k):
                forward(k).wait_recv()

        part[0, s, :, 0:cols] = lax.dot_general(
            rows[s * strip : cols, :], rows[0:cols, :], NT, preferred_element_type=jnp.float32
        ).astype(jnp.bfloat16)
        share(0, s).start()
        if s > 0:
            trace = settle(s - 1, trace)
        for level in range(1, levels):
            share(level - 1, s).wait_recv()
            part[level, s, :, 0:cols] = (
                part[level - 1, s, :, 0:cols].astype(jnp.float32)
                + got[level - 1, s, :, 0:cols].astype(jnp.float32)
            ).astype(jnp.bfloat16)
            share(level, s).start()
    trace = settle(strips - 1, trace)

    live_count = jnp.full((1, 1), live_ref[d], jnp.int32).astype(jnp.float32)
    scale_sq = 2.0 * trace / live_count
    shrink = 1.0 / scale_sq
    gain = (0.2 * math.sqrt(width_all)) / jnp.sqrt(scale_sq)

    @pl.loop(0, strips)
    def _(s):
        at = pl.ds(pl.multiple_of(s * strip, strip), strip)
        normed[at, :] = (gram[at, :] * shrink).astype(jnp.bfloat16)

    def update(s):
        at = pl.ds(pl.multiple_of(s * strip, strip), strip)
        square = lax.dot_general(normed[at, :], normed[...], NN, preferred_element_type=jnp.float32)
        mix = (2.0315 * square - 4.775 * normed[at, :].astype(jnp.float32)).astype(jnp.bfloat16)
        moved = lax.dot_general(mix, rows[...], NN, preferred_element_type=jnp.float32)
        upd[at, :] = ((3.4445 * rows[at, :].astype(jnp.float32) + moved) * gain).astype(jnp.bfloat16)

    if per == 1:
        @pl.loop(0, n - 1)
        def _(j):
            slot = far_first(j)
            update(slot)
            back(slot).start()

        update(0)
    else:
        @pl.loop(1, strips)
        def _(s):
            update(s)

            @pl.loop(0, per)
            def _(k):
                back(s * per + k).start()

        update(0)

        @pl.loop(1, per)
        def _(k):
            back(k).start()

    own_copy = pltpu.make_async_copy(upd.at[pl.ds(0, size)], out_ref.at[d], own_sem)
    own_copy.start()

    for s in range(strips):
        for level in range(levels):
            share(level, s).wait_send()

    @pl.loop(1, n)
    def _(k):
        forward(k).wait_send()

    @pl.loop(1, n)
    def _(k):
        back(k).wait_send()
        back_arrival(k).wait_recv()

    own_copy.wait()


def pick(values, index):
    out = jnp.int32(values[0]) if isinstance(values[0], int) else values[0]
    for k in range(1, len(values)):
        out = jnp.where(index == k, values[k], out)
    return out


def ranks(live_ref, matrices):
    lives = [live_ref[m] for m in range(matrices)]
    found = []
    for m in range(matrices):
        ahead = jnp.int32(0)
        for k in range(matrices):
            if k != m:
                before = lives[k] >= lives[m] if k < m else lives[k] > lives[m]
                ahead = ahead + jnp.where(before, 1, 0)
        found.append(ahead)
    return found


class Plan:
    def __init__(self, n, slots):
        self.ranks = [s[0] for s in slots]
        self.owners = [s[1] for s in slots]
        self.caps = [s[2] for s in slots]
        held = [[] for _ in range(n)]
        self.places = []
        for j, owner in enumerate(self.owners):
            self.places.append(len(held[owner]))
            held[owner].append(j)
        self.counts = [len(h) for h in held]
        self.most = max(self.counts)
        self.held = [[h[p] if p < len(h) else 0 for h in held] for p in range(self.most)]
        self.held_caps = [[self.caps[j] for j in row] for row in self.held]

    def sorted_caps(self):
        return [cap for _, cap in sorted(zip(self.ranks, self.caps))]


def sparse_kernel(
    plan, n, owners, width_all, live_ref, grad_ref, out_ref,
    stage, send, rows, gram, normed, upd, part, got, trace,
    load_sem, send_sem, recv_sem, psend_sem, precv_sem, usend_sem, urecv_sem, own_sem,
):
    d = lax.axis_index("dp")
    o = lax.axis_index("owner")
    matrices, size, width = stage.shape
    hidden = rows.shape[1]
    strip, strips = size, n
    levels = owners.bit_length() - 1

    def strip_at(t):
        return pl.ds(pl.multiple_of(t * size, size), size)

    def load(m):
        return pltpu.make_async_copy(grad_ref.at[m], stage.at[m], load_sem.at[m])

    def forward(j, owner, place):
        return pltpu.make_async_remote_copy(
            src_ref=send.at[j], dst_ref=rows.at[place, strip_at(d)],
            send_sem=send_sem.at[j], recv_sem=recv_sem.at[place, d],
            device_id={"dp": owner}, device_id_type=MESH,
        )

    def arrival(place, t):
        return pltpu.make_async_remote_copy(
            src_ref=send.at[0], dst_ref=rows.at[place, strip_at(t)],
            send_sem=send_sem.at[0], recv_sem=recv_sem.at[place, t],
            device_id={"dp": flip(d, 1, n)}, device_id_type=MESH,
        )

    def back(place, slot, t):
        return pltpu.make_async_remote_copy(
            src_ref=upd.at[place, strip_at(t)], dst_ref=out_ref.at[slot],
            send_sem=usend_sem.at[place, t], recv_sem=urecv_sem.at[slot],
            device_id={"dp": t}, device_id_type=MESH,
        )

    def back_arrival(slot):
        return pltpu.make_async_remote_copy(
            src_ref=upd.at[0, strip_at(0)], dst_ref=out_ref.at[slot],
            send_sem=usend_sem.at[0, 0], recv_sem=urecv_sem.at[slot],
            device_id={"dp": flip(d, 1, n)}, device_id_type=MESH,
        )

    def share(place, level, s):
        cols = (s + 1) * strip
        return pltpu.make_async_remote_copy(
            src_ref=part.at[place, level, s, :, pl.ds(0, cols)],
            dst_ref=got.at[place, level, s, :, pl.ds(0, cols)],
            send_sem=psend_sem.at[place, level, s],
            recv_sem=precv_sem.at[place, level, s],
            device_id={"owner": flip(o, 2**level, owners)},
            device_id_type=MESH,
        )

    @pl.loop(0, matrices)
    def _(m):
        load(m).start()

    barrier = pltpu.get_barrier_semaphore()

    @pl.loop(1, n)
    def _(k):
        pl.semaphore_signal(barrier, inc=1, device_id={"dp": flip(d, k, n)}, device_id_type=MESH)

    for level in range(levels):
        pl.semaphore_signal(
            barrier, inc=1, device_id={"owner": flip(o, 2**level, owners)}, device_id_type=MESH
        )

    place_of = ranks(live_ref, matrices)
    matrix_of = []
    for j in range(matrices):
        found = jnp.int32(0)
        for m in range(matrices):
            found = found + jnp.where(place_of[m] == plan.ranks[j], m, 0)
        matrix_of.append(found)

    row_index = d * size + lax.broadcasted_iota(jnp.int32, (size, width), 0)

    def narrow(m):
        return jnp.where(row_index < live_ref[m], stage[m], 0.0).astype(jnp.bfloat16)

    count = pick(plan.counts, d)

    def held_slot(place):
        return pick([pick(row, d) for row in plan.held], place)

    def held_cap(place):
        return pick([pick(row, d) for row in plan.held_caps], place)

    pl.semaphore_wait(barrier, n - 1 + levels)

    @pl.loop(0, matrices)
    def _(m):
        load(m).wait()

    @pl.loop(0, matrices)
    def _(j):
        owner, place, m = pick(plan.owners, j), pick(plan.places, j), pick(matrix_of, j)
        inside = d < pick(plan.caps, j)

        @pl.when(inside & (owner == d))
        def _():
            rows[place, strip_at(d), :] = narrow(m)

        @pl.when(inside & (owner != d))
        def _():
            send[j] = narrow(m)
            forward(j, owner, place).start()

    eye = (
        lax.broadcasted_iota(jnp.int32, (strip, strip), 0)
        == lax.broadcasted_iota(jnp.int32, (strip, strip), 1)
    )
    column_index = lax.broadcasted_iota(jnp.int32, (strip, hidden), 1)

    @pl.loop(0, count)
    def _(place):
        slot, cap = held_slot(place), held_cap(place)
        live_count = live_ref[pick(matrix_of, slot)]

        @pl.loop(cap, n)
        def _(t):
            rows[place, strip_at(t), :] = jnp.zeros((size, width), jnp.bfloat16)
            normed[strip_at(t), :] = jnp.zeros((strip, hidden), jnp.bfloat16)

        trace[...] = jnp.zeros_like(trace)

        def settle(s):
            at = s * strip
            cols = at + strip
            share(place, levels - 1, s).wait_recv()
            total = (
                part[place, levels - 1, s, :, 0:cols].astype(jnp.float32)
                + got[place, levels - 1, s, :, 0:cols].astype(jnp.float32)
            )
            gram[at:cols, 0:cols] = total
            for j in range(s):
                gram[j * strip : (j + 1) * strip, at:cols] = total[:, j * strip : (j + 1) * strip].T
            trace[...] += jnp.sum(jnp.where(eye, total[:, at:cols], 0.0), axis=0, keepdims=True)

        for s in range(strips + 1):
            cols = (s + 1) * strip

            if s < strips:

                @pl.when(s < cap)
                def _():
                    @pl.when(d != s)
                    def _():
                        arrival(place, s).wait_recv()

                    part[place, 0, s, :, 0:cols] = lax.dot_general(
                        rows[place, s * strip : cols, :], rows[place, 0:cols, :], NT,
                        preferred_element_type=jnp.float32,
                    ).astype(jnp.bfloat16)
                    share(place, 0, s).start()

            if s > 0:

                @pl.when(s <= cap)
                def _():
                    settle(s - 1)

            if s < strips:

                @pl.when(s < cap)
                def _():
                    for level in range(1, levels):
                        share(place, level - 1, s).wait_recv()
                        part[place, level, s, :, 0:cols] = (
                            part[place, level - 1, s, :, 0:cols].astype(jnp.float32)
                            + got[place, level - 1, s, :, 0:cols].astype(jnp.float32)
                        ).astype(jnp.bfloat16)
                        share(place, level, s).start()

        whole = jnp.sum(trace[...], keepdims=True)
        scale_sq = 2.0 * whole / jnp.full((1, 1), live_count, jnp.int32).astype(jnp.float32)
        shrink = 1.0 / scale_sq
        gain = (0.2 * math.sqrt(width_all)) / jnp.sqrt(scale_sq)

        @pl.loop(0, cap)
        def _(t):
            normed[strip_at(t), :] = jnp.where(
                column_index < cap * strip, gram[strip_at(t), :] * shrink, 0.0
            ).astype(jnp.bfloat16)

        def update(t):
            at = strip_at(t)
            square = lax.dot_general(normed[at, :], normed[...], NN, preferred_element_type=jnp.float32)
            mix = (2.0315 * square - 4.775 * normed[at, :].astype(jnp.float32)).astype(jnp.bfloat16)
            moved = lax.dot_general(mix, rows[place], NN, preferred_element_type=jnp.float32)
            upd[place, at, :] = (
                (3.4445 * rows[place, at, :].astype(jnp.float32) + moved) * gain
            ).astype(jnp.bfloat16)

        @pl.loop(0, n)
        def _(j):
            t = flip(d, pick([*range(n // 2, n), *range(1, n // 2), 0], j), n)

            @pl.when(t < cap)
            def _():
                update(t)

                @pl.when(t != d)
                def _():
                    back(place, slot, t).start()

        pltpu.make_async_copy(upd.at[place, strip_at(d)], out_ref.at[slot], own_sem.at[place]).start()

    @pl.loop(0, count)
    def _(place):
        slot, cap = held_slot(place), held_cap(place)
        for s in range(strips):

            @pl.when(s < cap)
            def _():
                for level in range(levels):
                    share(place, level, s).wait_send()

        @pl.loop(0, cap)
        def _(t):
            @pl.when(t != d)
            def _():
                back(place, slot, t).wait_send()

        pltpu.make_async_copy(upd.at[place, strip_at(d)], out_ref.at[slot], own_sem.at[place]).wait()

    @pl.loop(0, matrices)
    def _(j):
        owner, place = pick(plan.owners, j), pick(plan.places, j)

        @pl.when((d < pick(plan.caps, j)) & (owner != d))
        def _():
            forward(j, owner, place).wait_send()
            back_arrival(j).wait_recv()


def arrange_kernel(live_ref, slots_ref, out_ref):
    size, width = out_ref.shape[1:]
    row_index = lax.axis_index("dp") * size + lax.broadcasted_iota(jnp.int32, (size, width), 0)
    live = live_ref[pl.program_id(0)]
    out_ref[0] = jnp.where(row_index < live, slots_ref[0].astype(jnp.float32), 0.0).astype(jnp.bfloat16)


def plans_for(n, matrices, size):
    if size % 128 or n % 8 or matrices != n:
        return []
    quarter = n // 4
    above = [(r, 2 * quarter + r % quarter) for r in range(quarter)]
    below = [(r, quarter + (quarter - 1 - r % quarter)) for r in range(quarter, 2 * quarter)]
    lowest = []
    for k, r in enumerate(range(2 * quarter, n)):
        lowest.append((r, k % quarter if k < quarter else quarter - 1 - k % quarter))
    order = [pair for both in zip(above, below) for pair in both] + lowest
    plans = []
    for shares in CAPS:
        slots = [(r, owner, shares[r * len(shares) // n] * n // 8) for r, owner in order]
        plans.append(Plan(n, slots))
    return plans


CAPS = (
    (8, 8, 7, 7, 6, 5, 4, 3),
)


def solution(mesh):
    n, owners = mesh.shape["dp"], mesh.shape["owner"]
    dma = pltpu.SemaphoreType.DMA

    def dense(rows_live, gradients):
        matrices, size, width = gradients.shape
        hidden = size * n
        strip = max(size, min(128, hidden))
        strips = hidden // strip
        levels = owners.bit_length() - 1
        return pl.pallas_call(
            functools.partial(kernel, n, owners, width * owners),
            out_shape=jax.ShapeDtypeStruct((matrices, size, width), jnp.bfloat16),
            in_specs=[
                pl.BlockSpec(memory_space=pltpu.SMEM),
                pl.BlockSpec(memory_space=pl.ANY),
            ],
            out_specs=pl.BlockSpec(memory_space=pl.ANY),
            scratch_shapes=[
                pltpu.VMEM((n, size, width), jnp.float32),
                pltpu.VMEM((n, size, width), jnp.bfloat16),
                pltpu.VMEM((hidden, width), jnp.bfloat16),
                pltpu.VMEM((hidden, hidden), jnp.float32),
                pltpu.VMEM((hidden, hidden), jnp.bfloat16),
                pltpu.VMEM((hidden, width), jnp.bfloat16),
                pltpu.VMEM((levels, strips, strip, hidden), jnp.bfloat16),
                pltpu.VMEM((levels, strips, strip, hidden), jnp.bfloat16),
                dma((n,)), dma((n,)), dma((n,)),
                dma((levels, strips)), dma((levels, strips)),
                dma((n,)), dma((n,)), dma,
            ],
            compiler_params=pltpu.CompilerParams(
                collective_id=0, has_side_effects=True, vmem_limit_bytes=60 * 2**20
            ),
        )(rows_live, gradients)

    def sparse(plan, number, rows_live, gradients):
        matrices, size, width = gradients.shape
        hidden = size * n
        levels = owners.bit_length() - 1
        most = plan.most
        slots = pl.pallas_call(
            functools.partial(sparse_kernel, plan, n, owners, width * owners),
            out_shape=jax.ShapeDtypeStruct((matrices, size, width), jnp.bfloat16),
            in_specs=[
                pl.BlockSpec(memory_space=pltpu.SMEM),
                pl.BlockSpec(memory_space=pl.ANY),
            ],
            out_specs=pl.BlockSpec(memory_space=pl.ANY),
            scratch_shapes=[
                pltpu.VMEM((matrices, size, width), jnp.float32),
                pltpu.VMEM((matrices, size, width), jnp.bfloat16),
                pltpu.VMEM((most, hidden, width), jnp.bfloat16),
                pltpu.VMEM((hidden, hidden), jnp.float32),
                pltpu.VMEM((hidden, hidden), jnp.bfloat16),
                pltpu.VMEM((most, hidden, width), jnp.bfloat16),
                pltpu.VMEM((most, levels, n, size, hidden), jnp.bfloat16),
                pltpu.VMEM((most, levels, n, size, hidden), jnp.bfloat16),
                pltpu.VMEM((1, size), jnp.float32),
                dma((matrices,)), dma((matrices,)), dma((most, n)),
                dma((most, levels, n)), dma((most, levels, n)),
                dma((most, n)), dma((matrices,)), dma((most,)),
            ],
            compiler_params=pltpu.CompilerParams(
                collective_id=number, has_side_effects=True, vmem_limit_bytes=60 * 2**20
            ),
        )(rows_live, gradients)

        slot_of_rank = [plan.ranks.index(r) for r in range(matrices)]

        def source(m, live_ref):
            own = live_ref[m]
            rank = jnp.int32(0)
            for k in range(matrices):
                other = live_ref[k]
                rank = rank + jnp.where((other > own) | ((other == own) & (k < m)), 1, 0)
            return pick(slot_of_rank, rank), 0, 0

        return pl.pallas_call(
            arrange_kernel,
            out_shape=jax.ShapeDtypeStruct((matrices, size, width), jnp.bfloat16),
            grid_spec=pltpu.PrefetchScalarGridSpec(
                num_scalar_prefetch=1,
                grid=(matrices,),
                in_specs=[pl.BlockSpec((1, size, width), source)],
                out_specs=pl.BlockSpec((1, size, width), lambda m, live_ref: (m, 0, 0)),
            ),
        )(rows_live, slots)

    def body(gradients, rows_live):
        matrices, size, _ = gradients.shape
        plans = plans_for(n, matrices, size)
        if not plans:
            return dense(rows_live, gradients)
        caps = jnp.array([p.sorted_caps() for p in plans], jnp.int32) * size
        above = jnp.sum((rows_live[None, None, :] > caps[:, :, None]).astype(jnp.int32), axis=-1)
        misfit = jnp.any(above > jnp.arange(matrices, dtype=jnp.int32), axis=-1)
        index = jnp.int32(len(plans))
        for v in reversed(range(len(plans))):
            index = jnp.where(misfit[v], index, v)
        branches = [functools.partial(sparse, plan, 1 + v) for v, plan in enumerate(plans)]
        return lax.switch(index, branches + [dense], rows_live, gradients)

    return jax.shard_map(
        body,
        mesh=mesh,
        in_specs=(P(None, "dp", "owner"), P()),
        out_specs=P(None, "dp", "owner"),
        check_vma=False,
    )
```

```python
import functools
import math

import jax
import jax.numpy as jnp
from jax import lax
from jax.experimental import pallas as pl
from jax.experimental.pallas import tpu as pltpu
from jax.sharding import PartitionSpec as P

MESH = pl.DeviceIdType.MESH
NT = (((1,), (1,)), ((), ()))
NN = (((1,), (0,)), ((), ()))


def flip(index, bits, count):
    out, bit = 0, 1
    while bit < count:
        out = out + bit * (((index // bit) % 2 + (bits // bit) % 2) % 2)
        bit *= 2
    return out


def kernel(
    n, owners, width_all, live_ref, grad_ref, out_ref,
    stage, send, rows, gram, normed, upd, part, got,
    load_sem, send_sem, recv_sem, psend_sem, precv_sem, usend_sem, urecv_sem, own_sem,
):
    d = lax.axis_index("dp")
    o = lax.axis_index("owner")
    size, width = stage.shape[1], stage.shape[2]
    hidden = rows.shape[0]
    strip = max(size, min(128, hidden))
    strips = hidden // strip
    per = strip // size
    levels = owners.bit_length() - 1

    def far_first(j):
        return 1 + (j + n // 2 - 1) % (n - 1)

    def load(slot):
        return pltpu.make_async_copy(grad_ref.at[flip(d, slot, n)], stage.at[slot], load_sem.at[slot])

    def forward(slot):
        return pltpu.make_async_remote_copy(
            src_ref=send.at[slot],
            dst_ref=rows.at[pl.ds(pl.multiple_of(slot * size, size), size)],
            send_sem=send_sem.at[slot],
            recv_sem=recv_sem.at[slot],
            device_id={"dp": flip(d, slot, n)},
            device_id_type=MESH,
        )

    def back(slot):
        return pltpu.make_async_remote_copy(
            src_ref=upd.at[pl.ds(pl.multiple_of(slot * size, size), size)],
            dst_ref=out_ref.at[d],
            send_sem=usend_sem.at[slot],
            recv_sem=urecv_sem.at[slot],
            device_id={"dp": flip(d, slot, n)},
            device_id_type=MESH,
        )

    def back_arrival(slot):
        return pltpu.make_async_remote_copy(
            src_ref=upd.at[pl.ds(pl.multiple_of(slot * size, size), size)],
            dst_ref=out_ref.at[flip(d, slot, n)],
            send_sem=usend_sem.at[slot],
            recv_sem=urecv_sem.at[slot],
            device_id={"dp": flip(d, slot, n)},
            device_id_type=MESH,
        )

    def share(level, s):
        cols = (s + 1) * strip
        return pltpu.make_async_remote_copy(
            src_ref=part.at[level, s, :, pl.ds(0, cols)],
            dst_ref=got.at[level, s, :, pl.ds(0, cols)],
            send_sem=psend_sem.at[level, s],
            recv_sem=precv_sem.at[level, s],
            device_id={"owner": flip(o, 2**level, owners)},
            device_id_type=MESH,
        )

    @pl.loop(0, n - 1)
    def _(j):
        load(far_first(j)).start()

    load(0).start()

    barrier = pltpu.get_barrier_semaphore()

    @pl.loop(1, n)
    def _(k):
        pl.semaphore_signal(barrier, inc=1, device_id={"dp": flip(d, k, n)}, device_id_type=MESH)

    for level in range(levels):
        pl.semaphore_signal(
            barrier, inc=1, device_id={"owner": flip(o, 2**level, owners)}, device_id_type=MESH
        )
    pl.semaphore_wait(barrier, n - 1 + levels)

    row_index = d * size + lax.broadcasted_iota(jnp.int32, (size, width), 0)

    def narrow(slot):
        load(slot).wait()
        live = live_ref[flip(d, slot, n)]
        return jnp.where(row_index < live, stage[slot], 0.0).astype(jnp.bfloat16)

    @pl.loop(0, n - 1)
    def _(j):
        slot = far_first(j)
        send[slot] = narrow(slot)
        forward(slot).start()

    rows[pl.ds(0, size), :] = narrow(0)

    eye = (
        lax.broadcasted_iota(jnp.int32, (strip, strip), 0)
        == lax.broadcasted_iota(jnp.int32, (strip, strip), 1)
    )
    trace = jnp.zeros((1, 1), jnp.float32)

    def settle(s, trace):
        at = s * strip
        cols = at + strip
        share(levels - 1, s).wait_recv()
        total = (
            part[levels - 1, s, :, 0:cols].astype(jnp.float32)
            + got[levels - 1, s, :, 0:cols].astype(jnp.float32)
        )
        gram[at:cols, 0:cols] = total
        for j in range(s):
            gram[j * strip : (j + 1) * strip, at:cols] = total[:, j * strip : (j + 1) * strip].T
        own = jnp.where(eye, total[:, at:cols], 0.0)
        return trace + jnp.sum(own, keepdims=True)

    for s in range(strips):
        cols = (s + 1) * strip
        if s == 0:
            @pl.loop(1, per)
            def _(k):
                forward(k).wait_recv()
        else:
            @pl.loop(s * per, (s + 1) * per)
            def _(k):
                forward(k).wait_recv()

        part[0, s, :, 0:cols] = lax.dot_general(
            rows[s * strip : cols, :], rows[0:cols, :], NT, preferred_element_type=jnp.float32
        ).astype(jnp.bfloat16)
        share(0, s).start()
        if s > 0:
            trace = settle(s - 1, trace)
        for level in range(1, levels):
            share(level - 1, s).wait_recv()
            part[level, s, :, 0:cols] = (
                part[level - 1, s, :, 0:cols].astype(jnp.float32)
                + got[level - 1, s, :, 0:cols].astype(jnp.float32)
            ).astype(jnp.bfloat16)
            share(level, s).start()
    trace = settle(strips - 1, trace)

    live_count = jnp.full((1, 1), live_ref[d], jnp.int32).astype(jnp.float32)
    scale_sq = 2.0 * trace / live_count
    shrink = 1.0 / scale_sq
    gain = (0.2 * math.sqrt(width_all)) / jnp.sqrt(scale_sq)

    @pl.loop(0, strips)
    def _(s):
        at = pl.ds(pl.multiple_of(s * strip, strip), strip)
        normed[at, :] = (gram[at, :] * shrink).astype(jnp.bfloat16)

    def update(s):
        at = pl.ds(pl.multiple_of(s * strip, strip), strip)
        square = lax.dot_general(normed[at, :], normed[...], NN, preferred_element_type=jnp.float32)
        mix = (2.0315 * square - 4.775 * normed[at, :].astype(jnp.float32)).astype(jnp.bfloat16)
        moved = lax.dot_general(mix, rows[...], NN, preferred_element_type=jnp.float32)
        upd[at, :] = ((3.4445 * rows[at, :].astype(jnp.float32) + moved) * gain).astype(jnp.bfloat16)

    if per == 1:
        @pl.loop(0, n - 1)
        def _(j):
            slot = far_first(j)
            update(slot)
            back(slot).start()

        update(0)
    else:
        @pl.loop(1, strips)
        def _(s):
            update(s)

            @pl.loop(0, per)
            def _(k):
                back(s * per + k).start()

        update(0)

        @pl.loop(1, per)
        def _(k):
            back(k).start()

    own_copy = pltpu.make_async_copy(upd.at[pl.ds(0, size)], out_ref.at[d], own_sem)
    own_copy.start()

    for s in range(strips):
        for level in range(levels):
            share(level, s).wait_send()

    @pl.loop(1, n)
    def _(k):
        forward(k).wait_send()

    @pl.loop(1, n)
    def _(k):
        back(k).wait_send()
        back_arrival(k).wait_recv()

    own_copy.wait()


def pick(values, index):
    out = jnp.int32(values[0]) if isinstance(values[0], int) else values[0]
    for k in range(1, len(values)):
        out = jnp.where(index == k, values[k], out)
    return out


def ranks(live_ref, matrices):
    lives = [live_ref[m] for m in range(matrices)]
    found = []
    for m in range(matrices):
        ahead = jnp.int32(0)
        for k in range(matrices):
            if k != m:
                before = lives[k] >= lives[m] if k < m else lives[k] > lives[m]
                ahead = ahead + jnp.where(before, 1, 0)
        found.append(ahead)
    return found


class Plan:
    def __init__(self, n, slots, turned):
        self.turned = turned
        self.ranks = [s[0] for s in slots]
        self.owners = [s[1] for s in slots]
        self.caps = [s[2] for s in slots]
        held = [[] for _ in range(n)]
        self.places = []
        for j, owner in enumerate(self.owners):
            self.places.append(len(held[owner]))
            held[owner].append(j)
        self.counts = [len(h) for h in held]
        self.most = max(self.counts)
        self.held = [[h[p] if p < len(h) else 0 for h in held] for p in range(self.most)]
        self.held_caps = [[self.caps[j] for j in row] for row in self.held]

    def sorted_caps(self):
        return [cap for _, cap in sorted(zip(self.ranks, self.caps))]


def sparse_kernel(
    plan, n, owners, width_all, live_ref, grad_ref, out_ref,
    stage, send, rows, gram, normed, upd, part, sums, got, trace,
    load_sem, send_sem, recv_sem, psend_sem, precv_sem, usend_sem, urecv_sem, own_sem,
):
    d = lax.axis_index("dp")
    o = lax.axis_index("owner")
    matrices, size, width = stage.shape
    hidden = rows.shape[1]
    strip, strips, half = size, n, size // 2
    levels = owners.bit_length() - 1

    def strip_at(t):
        return pl.ds(pl.multiple_of(t * size, size), size)

    def load(m):
        return pltpu.make_async_copy(grad_ref.at[m], stage.at[m], load_sem.at[m])

    def part_at(t, halves):
        return pl.ds(pl.multiple_of(t * size, size), halves * half)

    def sent(cap, t, run):
        @pl.when(cap >= 2 * t + 2)
        def _():
            run(2)

        @pl.when(cap == 2 * t + 1)
        def _():
            run(1)

    def forward(j, owner, place, halves):
        return pltpu.make_async_remote_copy(
            src_ref=send.at[j, pl.ds(0, halves * half)], dst_ref=rows.at[place, part_at(d, halves)],
            send_sem=send_sem.at[j], recv_sem=recv_sem.at[place, d],
            device_id={"dp": owner}, device_id_type=MESH,
        )

    def arrival(place, t, halves):
        return pltpu.make_async_remote_copy(
            src_ref=send.at[0, pl.ds(0, halves * half)], dst_ref=rows.at[place, part_at(t, halves)],
            send_sem=send_sem.at[0], recv_sem=recv_sem.at[place, t],
            device_id={"dp": flip(d, 1, n)}, device_id_type=MESH,
        )

    def back(place, rank, t, halves):
        return pltpu.make_async_remote_copy(
            src_ref=upd.at[place, part_at(t, halves)], dst_ref=out_ref.at[rank, pl.ds(0, halves * half)],
            send_sem=usend_sem.at[place, t], recv_sem=urecv_sem.at[rank],
            device_id={"dp": t}, device_id_type=MESH,
        )

    def back_arrival(rank, halves):
        return pltpu.make_async_remote_copy(
            src_ref=upd.at[0, part_at(0, halves)], dst_ref=out_ref.at[rank, pl.ds(0, halves * half)],
            send_sem=usend_sem.at[0, 0], recv_sem=urecv_sem.at[rank],
            device_id={"dp": flip(d, 1, n)}, device_id_type=MESH,
        )

    mine = o % 2
    keep = pl.ds(pl.multiple_of(mine * half, half), half)
    give = pl.ds(pl.multiple_of((1 - mine) * half, half), half)

    def owner_copy(src, dst, sent_sem, received_sem, bit):
        return pltpu.make_async_remote_copy(
            src_ref=src, dst_ref=dst, send_sem=sent_sem, recv_sem=received_sem,
            device_id={"owner": flip(o, bit, owners)}, device_id_type=MESH,
        )

    def scatter(place, s):
        cols = pl.ds(0, (s + 1) * strip)
        return owner_copy(
            part.at[place, s, give, cols], got.at[place, 0, s, :, cols],
            psend_sem.at[place, 0, s], precv_sem.at[place, 0, s], 1,
        )

    def share(place, level, s):
        cols = pl.ds(0, (s + 1) * strip)
        return owner_copy(
            sums.at[place, level - 1, s, :, cols], got.at[place, level, s, :, cols],
            psend_sem.at[place, level, s], precv_sem.at[place, level, s], 2**level,
        )

    def gather(place, s):
        at = pl.ds(pl.multiple_of(s * strip + mine * half, half), half)
        here = gram.at[at, pl.ds(0, (s + 1) * strip)]
        return owner_copy(here, here, psend_sem.at[place, levels, s], precv_sem.at[place, levels, s], 1)

    @pl.loop(0, matrices)
    def _(m):
        load(m).start()

    barrier = pltpu.get_barrier_semaphore()

    @pl.loop(1, n)
    def _(k):
        pl.semaphore_signal(barrier, inc=1, device_id={"dp": flip(d, k, n)}, device_id_type=MESH)

    for level in range(levels):
        pl.semaphore_signal(
            barrier, inc=1, device_id={"owner": flip(o, 2**level, owners)}, device_id_type=MESH
        )

    place_of = ranks(live_ref, matrices)
    matrix_of = []
    for j in range(matrices):
        found = jnp.int32(0)
        for m in range(matrices):
            found = found + jnp.where(place_of[m] == plan.ranks[j], m, 0)
        matrix_of.append(found)

    row_index = d * size + lax.broadcasted_iota(jnp.int32, (size, width), 0)

    def narrow(m):
        return jnp.where(row_index < live_ref[m], stage[m], 0.0).astype(jnp.bfloat16)

    count = pick(plan.counts, d)

    def held_slot(place):
        return pick([pick(row, d) for row in plan.held], place)

    def held_cap(place):
        return pick([pick(row, d) for row in plan.held_caps], place)

    pl.semaphore_wait(barrier, n - 1 + levels)

    @pl.loop(0, matrices)
    def _(m):
        load(m).wait()

    @pl.loop(0, matrices)
    def _(i):
        j = (i + d) % matrices if plan.turned else matrices - 1 - i
        owner, place, m = pick(plan.owners, j), pick(plan.places, j), pick(matrix_of, j)
        cap = pick(plan.caps, j)
        inside = 2 * d < cap

        @pl.when(inside & (owner == d))
        def _():
            rows[place, strip_at(d), :] = narrow(m)

        @pl.when(inside & (owner != d))
        def _():
            send[j] = narrow(m)
            sent(cap, d, lambda halves: forward(j, owner, place, halves).start())

    eye = (
        lax.broadcasted_iota(jnp.int32, (strip, strip), 0)
        == lax.broadcasted_iota(jnp.int32, (strip, strip), 1)
    )
    column_index = lax.broadcasted_iota(jnp.int32, (strip, hidden), 1)

    @pl.loop(0, count)
    def _(place):
        slot, cap_halves = held_slot(place), held_cap(place)
        rank = pick(plan.ranks, slot)
        cap = (cap_halves + 1) // 2
        live_count = live_ref[pick(matrix_of, slot)]

        @pl.loop(cap_halves, 2 * n)
        def _(u):
            at = pl.ds(pl.multiple_of(u * half, half), half)
            rows[place, at, :] = jnp.zeros((half, width), jnp.bfloat16)

        @pl.loop(cap, n)
        def _(t):
            normed[strip_at(t), :] = jnp.zeros((strip, hidden), jnp.bfloat16)

        trace[...] = jnp.zeros_like(trace)

        def start(s):
            cols = (s + 1) * strip

            @pl.when(d != s)
            def _():
                sent(cap_halves, s, lambda halves: arrival(place, s, halves).wait_recv())

            part[place, s, :, 0:cols] = lax.dot_general(
                rows[place, s * strip : cols, :], rows[place, 0:cols, :], NT,
                preferred_element_type=jnp.float32,
            ).astype(jnp.bfloat16)
            scatter(place, s).start()

        def combine(level, s):
            cols = (s + 1) * strip
            if level == 0:
                scatter(place, s).wait_recv()
                own = part[place, s, keep, 0:cols]
            else:
                share(place, level, s).wait_recv()
                own = sums[place, level - 1, s, :, 0:cols]
            total = own.astype(jnp.float32) + got[place, level, s, :, 0:cols].astype(jnp.float32)
            if level < levels - 1:
                sums[place, level, s, :, 0:cols] = total.astype(jnp.bfloat16)
                share(place, level + 1, s).start()
            else:
                gram[pl.ds(pl.multiple_of(s * strip + mine * half, half), half), 0:cols] = total
                gather(place, s).start()

        def settle(s):
            at = s * strip
            cols = at + strip
            gather(place, s).wait_recv()
            for j in range(s):
                gram[j * strip : (j + 1) * strip, at:cols] = gram[at:cols, j * strip : (j + 1) * strip].T
            trace[...] += jnp.sum(jnp.where(eye, gram[at:cols, at:cols], 0.0), axis=0, keepdims=True)

        steps = [start, *[functools.partial(combine, level) for level in range(levels)], settle]
        lags = range(levels + 2)
        for at_step in range(strips + max(lags)):
            for run, lag in zip(steps, lags):
                s = at_step - lag
                if 0 <= s < strips:
                    pl.when(s < cap)(functools.partial(run, s))

        whole = jnp.sum(trace[...], keepdims=True)
        scale_sq = 2.0 * whole / jnp.full((1, 1), live_count, jnp.int32).astype(jnp.float32)
        shrink = 1.0 / scale_sq
        gain = (0.2 * math.sqrt(width_all)) / jnp.sqrt(scale_sq)

        for s in range(strips):
            pl.when(s < cap)(gather(place, s).wait_send)

        @pl.loop(0, cap)
        def _(t):
            normed[strip_at(t), :] = jnp.where(
                column_index < cap * strip, gram[strip_at(t), :] * shrink, 0.0
            ).astype(jnp.bfloat16)

        def update(t):
            at = strip_at(t)
            square = lax.dot_general(normed[at, :], normed[...], NN, preferred_element_type=jnp.float32)
            mix = (2.0315 * square - 4.775 * normed[at, :].astype(jnp.float32)).astype(jnp.bfloat16)
            moved = lax.dot_general(mix, rows[place], NN, preferred_element_type=jnp.float32)
            upd[place, at, :] = (
                (3.4445 * rows[place, at, :].astype(jnp.float32) + moved) * gain
            ).astype(jnp.bfloat16)

        @pl.loop(0, n)
        def _(j):
            t = flip(d, pick([*range(n // 2, n), *range(1, n // 2), 0], j), n)

            @pl.when(t < cap)
            def _():
                update(t)

                @pl.when(t != d)
                def _():
                    sent(cap_halves, t, lambda halves: back(place, rank, t, halves).start())

        pltpu.make_async_copy(upd.at[place, strip_at(d)], out_ref.at[rank], own_sem.at[place]).start()

    @pl.loop(0, count)
    def _(place):
        slot, cap_halves = held_slot(place), held_cap(place)
        rank = pick(plan.ranks, slot)
        cap = (cap_halves + 1) // 2
        for s in range(strips):

            @pl.when(s < cap)
            def _():
                scatter(place, s).wait_send()
                for level in range(1, levels):
                    share(place, level, s).wait_send()

        @pl.loop(0, cap)
        def _(t):
            @pl.when(t != d)
            def _():
                sent(cap_halves, t, lambda halves: back(place, rank, t, halves).wait_send())

        pltpu.make_async_copy(upd.at[place, strip_at(d)], out_ref.at[rank], own_sem.at[place]).wait()

    @pl.loop(0, matrices)
    def _(j):
        owner, place, rank = pick(plan.owners, j), pick(plan.places, j), pick(plan.ranks, j)

        @pl.when(owner != d)
        def _():
            def run(halves):
                forward(j, owner, place, halves).wait_send()
                back_arrival(rank, halves).wait_recv()

            sent(pick(plan.caps, j), d, run)


def choose_kernel(caps, half, live_ref, index_ref):
    matrices = len(caps[0])
    place_of = ranks(live_ref, matrices)
    index = jnp.int32(len(caps))
    for v in reversed(range(len(caps))):
        over = jnp.int32(0)
        for m in range(matrices):
            over = over + jnp.where(live_ref[m] > pick(caps[v], place_of[m]) * half, 1, 0)
        index = jnp.where(over == 0, v, index)
    index_ref[0] = index


def arrange_kernel(ranked, live_ref, index_ref, slots_ref, out_ref, fetched, placed, in_sem, out_sem):
    matrices, size, width = fetched.shape
    row_index = lax.axis_index("dp") * size + lax.broadcasted_iota(jnp.int32, (size, width), 0)
    place_of = ranks(live_ref, matrices)

    def fetch(m, source):
        return pltpu.make_async_copy(slots_ref.at[source], fetched.at[m], in_sem.at[m])

    def put(m):
        return pltpu.make_async_copy(placed.at[m], out_ref.at[m], out_sem.at[m])

    for m in range(matrices):
        fetch(m, jnp.where(index_ref[0] < ranked, place_of[m], m)).start()

    @pl.loop(0, matrices)
    def _(m):
        fetch(m, m).wait()
        kept = jnp.where(row_index < live_ref[m], fetched[m].astype(jnp.float32), 0.0)
        placed[m] = kept.astype(jnp.bfloat16)
        put(m).start()

    @pl.loop(0, matrices)
    def _(m):
        put(m).wait()


PLANS = (
    ((5, 4, 2, 3, 1, 0, 0, 1), (16, 16, 16, 12, 11, 8, 8, 4), False),
    ((5, 4, 2, 3, 1, 0, 0, 1), (16, 16, 16, 13, 12, 9, 8, 4), True),
    ((5, 4, 3, 2, 0, 1, 2, 1), (16, 16, 16, 15, 12, 12, 8, 4), False),
    ((4, 5, 2, 3, 1, 2, 0, 0), (16, 16, 16, 16, 13, 12, 9, 4), False),
)


def plans_for(n, matrices, size):
    if size % 128 or n % 8 or matrices != n:
        return []
    many = n // 8
    plans = []
    for owners, caps, turned in PLANS:
        slots = []
        for share in range(8):
            for k in range(many):
                slots.append((share * many + k, owners[share] * many + k, caps[share] * many))
        plans.append(Plan(n, slots, turned))
    return plans


def solution(mesh):
    n, owners = mesh.shape["dp"], mesh.shape["owner"]
    dma = pltpu.SemaphoreType.DMA

    def dense(rows_live, gradients):
        matrices, size, width = gradients.shape
        hidden = size * n
        strip = max(size, min(128, hidden))
        strips = hidden // strip
        levels = owners.bit_length() - 1
        return pl.pallas_call(
            functools.partial(kernel, n, owners, width * owners),
            out_shape=jax.ShapeDtypeStruct((matrices, size, width), jnp.bfloat16),
            in_specs=[
                pl.BlockSpec(memory_space=pltpu.SMEM),
                pl.BlockSpec(memory_space=pl.ANY),
            ],
            out_specs=pl.BlockSpec(memory_space=pl.ANY),
            scratch_shapes=[
                pltpu.VMEM((n, size, width), jnp.float32),
                pltpu.VMEM((n, size, width), jnp.bfloat16),
                pltpu.VMEM((hidden, width), jnp.bfloat16),
                pltpu.VMEM((hidden, hidden), jnp.float32),
                pltpu.VMEM((hidden, hidden), jnp.bfloat16),
                pltpu.VMEM((hidden, width), jnp.bfloat16),
                pltpu.VMEM((levels, strips, strip, hidden), jnp.bfloat16),
                pltpu.VMEM((levels, strips, strip, hidden), jnp.bfloat16),
                dma((n,)), dma((n,)), dma((n,)),
                dma((levels, strips)), dma((levels, strips)),
                dma((n,)), dma((n,)), dma,
            ],
            compiler_params=pltpu.CompilerParams(
                collective_id=0, has_side_effects=True, vmem_limit_bytes=60 * 2**20
            ),
        )(rows_live, gradients)

    def sparse(plan, number, rows_live, gradients):
        matrices, size, width = gradients.shape
        hidden = size * n
        levels = owners.bit_length() - 1
        most = plan.most
        return pl.pallas_call(
            functools.partial(sparse_kernel, plan, n, owners, width * owners),
            out_shape=jax.ShapeDtypeStruct((matrices, size, width), jnp.bfloat16),
            in_specs=[
                pl.BlockSpec(memory_space=pltpu.SMEM),
                pl.BlockSpec(memory_space=pl.ANY),
            ],
            out_specs=pl.BlockSpec(memory_space=pl.ANY),
            scratch_shapes=[
                pltpu.VMEM((matrices, size, width), jnp.float32),
                pltpu.VMEM((matrices, size, width), jnp.bfloat16),
                pltpu.VMEM((most, hidden, width), jnp.bfloat16),
                pltpu.VMEM((hidden, hidden), jnp.float32),
                pltpu.VMEM((hidden, hidden), jnp.bfloat16),
                pltpu.VMEM((most, hidden, width), jnp.bfloat16),
                pltpu.VMEM((most, n, size, hidden), jnp.bfloat16),
                pltpu.VMEM((most, levels - 1, n, size // 2, hidden), jnp.bfloat16),
                pltpu.VMEM((most, levels, n, size // 2, hidden), jnp.bfloat16),
                pltpu.VMEM((1, size), jnp.float32),
                dma((matrices,)), dma((matrices,)), dma((most, n)),
                dma((most, levels + 1, n)), dma((most, levels + 1, n)),
                dma((most, n)), dma((matrices,)), dma((most,)),
            ],
            compiler_params=pltpu.CompilerParams(
                collective_id=number, has_side_effects=True, vmem_limit_bytes=60 * 2**20
            ),
        )(rows_live, gradients)

    def body(gradients, rows_live):
        matrices, size, _ = gradients.shape
        plans = plans_for(n, matrices, size) if owners > 2 else []
        if not plans:
            return dense(rows_live, gradients)
        smem, anywhere = pl.BlockSpec(memory_space=pltpu.SMEM), pl.BlockSpec(memory_space=pl.ANY)
        index = pl.pallas_call(
            functools.partial(choose_kernel, [p.sorted_caps() for p in plans], size // 2),
            out_shape=jax.ShapeDtypeStruct((1,), jnp.int32),
            in_specs=[smem],
            out_specs=smem,
        )(rows_live)
        branches = [functools.partial(sparse, plan, 1 + v) for v, plan in enumerate(plans)]
        slots = lax.switch(index[0], branches + [dense], rows_live, gradients)
        return pl.pallas_call(
            functools.partial(arrange_kernel, len(plans)),
            out_shape=jax.ShapeDtypeStruct(slots.shape, slots.dtype),
            in_specs=[smem, smem, anywhere],
            out_specs=anywhere,
            scratch_shapes=[
                pltpu.VMEM(slots.shape, slots.dtype),
                pltpu.VMEM(slots.shape, slots.dtype),
                dma((matrices,)), dma((matrices,)),
            ],
        )(rows_live, index, slots)

    return jax.shard_map(
        body,
        mesh=mesh,
        in_specs=(P(None, "dp", "owner"), P()),
        out_specs=P(None, "dp", "owner"),
        check_vma=False,
    )
```

```python
import functools
import math

import jax
import jax.numpy as jnp
from jax import lax
from jax.experimental import pallas as pl
from jax.experimental.pallas import tpu as pltpu
from jax.sharding import PartitionSpec as P

MESH = pl.DeviceIdType.MESH
NT = (((1,), (1,)), ((), ()))
NN = (((1,), (0,)), ((), ()))


def flip(index, bits, count):
    out, bit = 0, 1
    while bit < count:
        out = out + bit * (((index // bit) % 2 + (bits // bit) % 2) % 2)
        bit *= 2
    return out


def kernel(
    n, owners, width_all, live_ref, grad_ref, out_ref,
    stage, send, rows, gram, normed, upd, part, got,
    load_sem, send_sem, recv_sem, psend_sem, precv_sem, usend_sem, urecv_sem, own_sem,
):
    d = lax.axis_index("dp")
    o = lax.axis_index("owner")
    size, width = stage.shape[1], stage.shape[2]
    hidden = rows.shape[0]
    strip = max(size, min(128, hidden))
    strips = hidden // strip
    per = strip // size
    levels = owners.bit_length() - 1

    def far_first(j):
        return 1 + (j + n // 2 - 1) % (n - 1)

    def load(slot):
        return pltpu.make_async_copy(grad_ref.at[flip(d, slot, n)], stage.at[slot], load_sem.at[slot])

    def forward(slot):
        return pltpu.make_async_remote_copy(
            src_ref=send.at[slot],
            dst_ref=rows.at[pl.ds(pl.multiple_of(slot * size, size), size)],
            send_sem=send_sem.at[slot],
            recv_sem=recv_sem.at[slot],
            device_id={"dp": flip(d, slot, n)},
            device_id_type=MESH,
        )

    def back(slot):
        return pltpu.make_async_remote_copy(
            src_ref=upd.at[pl.ds(pl.multiple_of(slot * size, size), size)],
            dst_ref=out_ref.at[d],
            send_sem=usend_sem.at[slot],
            recv_sem=urecv_sem.at[slot],
            device_id={"dp": flip(d, slot, n)},
            device_id_type=MESH,
        )

    def back_arrival(slot):
        return pltpu.make_async_remote_copy(
            src_ref=upd.at[pl.ds(pl.multiple_of(slot * size, size), size)],
            dst_ref=out_ref.at[flip(d, slot, n)],
            send_sem=usend_sem.at[slot],
            recv_sem=urecv_sem.at[slot],
            device_id={"dp": flip(d, slot, n)},
            device_id_type=MESH,
        )

    def share(level, s):
        cols = (s + 1) * strip
        return pltpu.make_async_remote_copy(
            src_ref=part.at[level, s, :, pl.ds(0, cols)],
            dst_ref=got.at[level, s, :, pl.ds(0, cols)],
            send_sem=psend_sem.at[level, s],
            recv_sem=precv_sem.at[level, s],
            device_id={"owner": flip(o, 2**level, owners)},
            device_id_type=MESH,
        )

    @pl.loop(0, n - 1)
    def _(j):
        load(far_first(j)).start()

    load(0).start()

    barrier = pltpu.get_barrier_semaphore()

    @pl.loop(1, n)
    def _(k):
        pl.semaphore_signal(barrier, inc=1, device_id={"dp": flip(d, k, n)}, device_id_type=MESH)

    for level in range(levels):
        pl.semaphore_signal(
            barrier, inc=1, device_id={"owner": flip(o, 2**level, owners)}, device_id_type=MESH
        )
    pl.semaphore_wait(barrier, n - 1 + levels)

    row_index = d * size + lax.broadcasted_iota(jnp.int32, (size, width), 0)

    def narrow(slot):
        load(slot).wait()
        live = live_ref[flip(d, slot, n)]
        return jnp.where(row_index < live, stage[slot], 0.0).astype(jnp.bfloat16)

    @pl.loop(0, n - 1)
    def _(j):
        slot = far_first(j)
        send[slot] = narrow(slot)
        forward(slot).start()

    rows[pl.ds(0, size), :] = narrow(0)

    eye = (
        lax.broadcasted_iota(jnp.int32, (strip, strip), 0)
        == lax.broadcasted_iota(jnp.int32, (strip, strip), 1)
    )
    trace = jnp.zeros((1, 1), jnp.float32)

    def settle(s, trace):
        at = s * strip
        cols = at + strip
        share(levels - 1, s).wait_recv()
        total = (
            part[levels - 1, s, :, 0:cols].astype(jnp.float32)
            + got[levels - 1, s, :, 0:cols].astype(jnp.float32)
        )
        gram[at:cols, 0:cols] = total
        for j in range(s):
            gram[j * strip : (j + 1) * strip, at:cols] = total[:, j * strip : (j + 1) * strip].T
        own = jnp.where(eye, total[:, at:cols], 0.0)
        return trace + jnp.sum(own, keepdims=True)

    for s in range(strips):
        cols = (s + 1) * strip
        if s == 0:
            @pl.loop(1, per)
            def _(k):
                forward(k).wait_recv()
        else:
            @pl.loop(s * per, (s + 1) * per)
            def _(k):
                forward(k).wait_recv()

        part[0, s, :, 0:cols] = lax.dot_general(
            rows[s * strip : cols, :], rows[0:cols, :], NT, preferred_element_type=jnp.float32
        ).astype(jnp.bfloat16)
        share(0, s).start()
        if s > 0:
            trace = settle(s - 1, trace)
        for level in range(1, levels):
            share(level - 1, s).wait_recv()
            part[level, s, :, 0:cols] = (
                part[level - 1, s, :, 0:cols].astype(jnp.float32)
                + got[level - 1, s, :, 0:cols].astype(jnp.float32)
            ).astype(jnp.bfloat16)
            share(level, s).start()
    trace = settle(strips - 1, trace)

    live_count = jnp.full((1, 1), live_ref[d], jnp.int32).astype(jnp.float32)
    scale_sq = 2.0 * trace / live_count
    shrink = 1.0 / scale_sq
    gain = (0.2 * math.sqrt(width_all)) / jnp.sqrt(scale_sq)

    @pl.loop(0, strips)
    def _(s):
        at = pl.ds(pl.multiple_of(s * strip, strip), strip)
        normed[at, :] = (gram[at, :] * shrink).astype(jnp.bfloat16)

    def update(s):
        at = pl.ds(pl.multiple_of(s * strip, strip), strip)
        square = lax.dot_general(normed[at, :], normed[...], NN, preferred_element_type=jnp.float32)
        mix = (2.0315 * square - 4.775 * normed[at, :].astype(jnp.float32)).astype(jnp.bfloat16)
        moved = lax.dot_general(mix, rows[...], NN, preferred_element_type=jnp.float32)
        upd[at, :] = ((3.4445 * rows[at, :].astype(jnp.float32) + moved) * gain).astype(jnp.bfloat16)

    if per == 1:
        @pl.loop(0, n - 1)
        def _(j):
            slot = far_first(j)
            update(slot)
            back(slot).start()

        update(0)
    else:
        @pl.loop(1, strips)
        def _(s):
            update(s)

            @pl.loop(0, per)
            def _(k):
                back(s * per + k).start()

        update(0)

        @pl.loop(1, per)
        def _(k):
            back(k).start()

    own_copy = pltpu.make_async_copy(upd.at[pl.ds(0, size)], out_ref.at[d], own_sem)
    own_copy.start()

    for s in range(strips):
        for level in range(levels):
            share(level, s).wait_send()

    @pl.loop(1, n)
    def _(k):
        forward(k).wait_send()

    @pl.loop(1, n)
    def _(k):
        back(k).wait_send()
        back_arrival(k).wait_recv()

    own_copy.wait()


def pick(values, index):
    out = jnp.int32(values[0]) if isinstance(values[0], int) else values[0]
    for k in range(1, len(values)):
        out = jnp.where(index == k, values[k], out)
    return out


def pick2(rows, row, index):
    return pick([pick(values, index) for values in rows], row)


def ranks(live_ref, matrices):
    lives = [live_ref[m] for m in range(matrices)]
    found = []
    for m in range(matrices):
        ahead = jnp.int32(0)
        for k in range(matrices):
            if k != m:
                before = lives[k] >= lives[m] if k < m else lives[k] > lives[m]
                ahead = ahead + jnp.where(before, 1, 0)
        found.append(ahead)
    return found


class Plan:
    def __init__(self, n, slots, small_first):
        self.ranks = [s[0] for s in slots]
        self.owners = [s[1] for s in slots]
        self.caps = [s[2] for s in slots]

        def late(owner, t):
            far, other = (owner ^ t) >= n // 2, (owner ^ t) % 2
            return (far and other, far, owner ^ t)

        held = [[] for _ in range(n)]
        self.places, self.blocks, self.halves, self.positions = [], [], [], []
        for j in reversed(range(len(slots))) if small_first else range(len(slots)):
            held[self.owners[j]].append(j)
        for j, (owner, cap) in enumerate(zip(self.owners, self.caps)):
            self.places.append(held[owner].index(j))
            blocks = sorted(range(n), key=lambda t: (2 * t >= cap, late(owner, t)))
            self.blocks.append(blocks)
            self.halves.append([min(2, max(0, cap - 2 * t)) for t in blocks])
            self.positions.append([blocks.index(t) for t in range(n)])
        self.orders = [
            sorted(range(len(slots)), key=lambda j: (late(self.owners[j], t)[0], -j)) for t in range(n)
        ]
        self.counts = [len(h) for h in held]
        self.most = max(self.counts)
        self.held = [[h[p] if p < len(h) else 0 for h in held] for p in range(self.most)]
        self.held_caps = [[self.caps[j] for j in row] for row in self.held]

    def sorted_caps(self):
        return [cap for _, cap in sorted(zip(self.ranks, self.caps))]


def sparse_kernel(
    plan, n, owners, width_all, live_ref, grad_ref, out_ref,
    stage, send, rows, gram, normed, upd, part, sums, got, trace,
    load_sem, send_sem, recv_sem, psend_sem, precv_sem, usend_sem, urecv_sem, own_sem,
):
    d = lax.axis_index("dp")
    o = lax.axis_index("owner")
    matrices, size, width = stage.shape
    hidden = rows.shape[1]
    strip, strips, half = size, n, size // 2
    levels = owners.bit_length() - 1

    def strip_at(t):
        return pl.ds(pl.multiple_of(t * size, size), size)

    def load(m):
        return pltpu.make_async_copy(grad_ref.at[m], stage.at[m], load_sem.at[m])

    def part_at(t, halves):
        return pl.ds(pl.multiple_of(t * size, size), halves * half)

    def sent(halves, run):
        pl.when(halves == 2)(functools.partial(run, 2))
        pl.when(halves == 1)(functools.partial(run, 1))

    def forward(j, owner, place, position, halves):
        return pltpu.make_async_remote_copy(
            src_ref=send.at[j, pl.ds(0, halves * half)], dst_ref=rows.at[place, part_at(position, halves)],
            send_sem=send_sem.at[j], recv_sem=recv_sem.at[place, position],
            device_id={"dp": owner}, device_id_type=MESH,
        )

    def back(place, rank, p, t, halves):
        return pltpu.make_async_remote_copy(
            src_ref=upd.at[place, part_at(p, halves)], dst_ref=out_ref.at[rank, pl.ds(0, halves * half)],
            send_sem=usend_sem.at[place, p], recv_sem=urecv_sem.at[rank],
            device_id={"dp": t}, device_id_type=MESH,
        )

    mine = o % 2
    keep = pl.ds(pl.multiple_of(mine * half, half), half)
    give = pl.ds(pl.multiple_of((1 - mine) * half, half), half)

    def owner_copy(src, dst, sent_sem, received_sem, bit):
        return pltpu.make_async_remote_copy(
            src_ref=src, dst_ref=dst, send_sem=sent_sem, recv_sem=received_sem,
            device_id={"owner": flip(o, bit, owners)}, device_id_type=MESH,
        )

    def scatter(place, s):
        cols = pl.ds(0, (s + 1) * strip)
        return owner_copy(
            part.at[place, s, give, cols], got.at[place, 0, s, :, cols],
            psend_sem.at[place, 0, s], precv_sem.at[place, 0, s], 1,
        )

    def share(place, level, s):
        cols = pl.ds(0, (s + 1) * strip)
        return owner_copy(
            sums.at[place, level - 1, s, :, cols], got.at[place, level, s, :, cols],
            psend_sem.at[place, level, s], precv_sem.at[place, level, s], 2**level,
        )

    def gather(place, s):
        at = pl.ds(pl.multiple_of(s * strip + mine * half, half), half)
        here = gram.at[at, pl.ds(0, (s + 1) * strip)]
        return owner_copy(here, here, psend_sem.at[place, levels, s], precv_sem.at[place, levels, s], 1)

    @pl.loop(0, matrices)
    def _(m):
        load(m).start()

    barrier = pltpu.get_barrier_semaphore()

    @pl.loop(1, n)
    def _(k):
        pl.semaphore_signal(barrier, inc=1, device_id={"dp": flip(d, k, n)}, device_id_type=MESH)

    for level in range(levels):
        pl.semaphore_signal(
            barrier, inc=1, device_id={"owner": flip(o, 2**level, owners)}, device_id_type=MESH
        )

    place_of = ranks(live_ref, matrices)
    matrix_of = []
    for j in range(matrices):
        found = jnp.int32(0)
        for m in range(matrices):
            found = found + jnp.where(place_of[m] == plan.ranks[j], m, 0)
        matrix_of.append(found)

    row_index = d * size + lax.broadcasted_iota(jnp.int32, (size, width), 0)

    def narrow(m):
        return jnp.where(row_index < live_ref[m], stage[m], 0.0).astype(jnp.bfloat16)

    count = pick(plan.counts, d)

    def held_slot(place):
        return pick([pick(row, d) for row in plan.held], place)

    def held_cap(place):
        return pick([pick(row, d) for row in plan.held_caps], place)

    pl.semaphore_wait(barrier, n - 1 + levels)

    @pl.loop(0, matrices)
    def _(m):
        load(m).wait()

    @pl.loop(0, matrices)
    def _(i):
        j = pick2(plan.orders, d, i)
        owner, place, m = pick(plan.owners, j), pick(plan.places, j), pick(matrix_of, j)
        position = pick2(plan.positions, j, d)
        halves_sent = pick2(plan.halves, j, position)
        inside = halves_sent > 0

        @pl.when(inside & (owner == d))
        def _():
            rows[place, 0:size, :] = narrow(m)

        @pl.when(inside & (owner != d))
        def _():
            send[j] = narrow(m)
            sent(halves_sent, lambda halves: forward(j, owner, place, position, halves).start())

    eye = (
        lax.broadcasted_iota(jnp.int32, (strip, strip), 0)
        == lax.broadcasted_iota(jnp.int32, (strip, strip), 1)
    )
    column_index = lax.broadcasted_iota(jnp.int32, (strip, hidden), 1)

    @pl.loop(0, count)
    def _(place):
        slot, cap_halves = held_slot(place), held_cap(place)
        rank = pick(plan.ranks, slot)
        cap = (cap_halves + 1) // 2
        live_count = live_ref[pick(matrix_of, slot)]

        @pl.loop(0, n)
        def _(p):
            halves = pick2(plan.halves, slot, p)
            for k in range(2):

                @pl.when(halves <= k)
                def _():
                    at = pl.ds(pl.multiple_of(p * size + k * half, half), half)
                    rows[place, at, :] = jnp.zeros((half, width), jnp.bfloat16)

        @pl.loop(cap, n)
        def _(t):
            normed[strip_at(t), :] = jnp.zeros((strip, hidden), jnp.bfloat16)

        trace[...] = jnp.zeros_like(trace)

        def start(s):
            cols = (s + 1) * strip

            if s > 0:
                sent(
                    pick([halves[s] for halves in plan.halves], slot),
                    lambda halves: forward(0, flip(d, 1, n), place, s, halves).wait_recv(),
                )

            part[place, s, :, 0:cols] = lax.dot_general(
                rows[place, s * strip : cols, :], rows[place, 0:cols, :], NT,
                preferred_element_type=jnp.float32,
            ).astype(jnp.bfloat16)
            scatter(place, s).start()

        def combine(level, s):
            cols = (s + 1) * strip
            if level == 0:
                scatter(place, s).wait_recv()
                own = part[place, s, keep, 0:cols]
            else:
                share(place, level, s).wait_recv()
                own = sums[place, level - 1, s, :, 0:cols]
            total = own.astype(jnp.float32) + got[place, level, s, :, 0:cols].astype(jnp.float32)
            if level < levels - 1:
                sums[place, level, s, :, 0:cols] = total.astype(jnp.bfloat16)
                share(place, level + 1, s).start()
            else:
                gram[pl.ds(pl.multiple_of(s * strip + mine * half, half), half), 0:cols] = total
                gather(place, s).start()

        def settle(s):
            at = s * strip
            cols = at + strip
            gather(place, s).wait_recv()
            for j in range(s):
                gram[j * strip : (j + 1) * strip, at:cols] = gram[at:cols, j * strip : (j + 1) * strip].T
            trace[...] += jnp.sum(jnp.where(eye, gram[at:cols, at:cols], 0.0), axis=0, keepdims=True)

        steps = [start, *[functools.partial(combine, level) for level in range(levels)], settle]
        lags = range(levels + 2)
        for at_step in range(strips + max(lags)):
            for run, lag in zip(steps, lags):
                s = at_step - lag
                if 0 <= s < strips:
                    pl.when(s < cap)(functools.partial(run, s))

        whole = jnp.sum(trace[...], keepdims=True)
        scale_sq = 2.0 * whole / jnp.full((1, 1), live_count, jnp.int32).astype(jnp.float32)
        shrink = 1.0 / scale_sq
        gain = (0.2 * math.sqrt(width_all)) / jnp.sqrt(scale_sq)

        for s in range(strips):
            pl.when(s < cap)(gather(place, s).wait_send)

        @pl.loop(0, cap)
        def _(t):
            normed[strip_at(t), :] = jnp.where(
                column_index < cap * strip, gram[strip_at(t), :] * shrink, 0.0
            ).astype(jnp.bfloat16)

        def update(t):
            at = strip_at(t)
            square = lax.dot_general(normed[at, :], normed[...], NN, preferred_element_type=jnp.float32)
            mix = (2.0315 * square - 4.775 * normed[at, :].astype(jnp.float32)).astype(jnp.bfloat16)
            moved = lax.dot_general(mix, rows[place], NN, preferred_element_type=jnp.float32)
            upd[place, at, :] = (
                (3.4445 * rows[place, at, :].astype(jnp.float32) + moved) * gain
            ).astype(jnp.bfloat16)

        @pl.loop(0, cap)
        def _(k):
            p = cap - 1 - k
            t = pick2(plan.blocks, slot, p)
            update(p)

            @pl.when(p > 0)
            def _():
                sent(pick2(plan.halves, slot, p), lambda halves: back(place, rank, p, t, halves).start())

        pltpu.make_async_copy(upd.at[place, pl.ds(0, size)], out_ref.at[rank], own_sem.at[place]).start()

    @pl.loop(0, count)
    def _(place):
        slot, cap_halves = held_slot(place), held_cap(place)
        rank = pick(plan.ranks, slot)
        cap = (cap_halves + 1) // 2
        for s in range(strips):

            @pl.when(s < cap)
            def _():
                scatter(place, s).wait_send()
                for level in range(1, levels):
                    share(place, level, s).wait_send()

        @pl.loop(1, cap)
        def _(p):
            t = pick2(plan.blocks, slot, p)
            sent(pick2(plan.halves, slot, p), lambda halves: back(place, rank, p, t, halves).wait_send())

        pltpu.make_async_copy(upd.at[place, pl.ds(0, size)], out_ref.at[rank], own_sem.at[place]).wait()

    @pl.loop(0, matrices)
    def _(j):
        owner, place, rank = pick(plan.owners, j), pick(plan.places, j), pick(plan.ranks, j)
        position = pick2(plan.positions, j, d)

        @pl.when(owner != d)
        def _():
            def run(halves):
                forward(j, owner, place, position, halves).wait_send()
                back(0, rank, 0, flip(d, 1, n), halves).wait_recv()

            sent(pick2(plan.halves, j, position), run)


def choose_kernel(caps, half, live_ref, index_ref):
    matrices = len(caps[0])
    place_of = ranks(live_ref, matrices)
    index = jnp.int32(len(caps))
    for v in reversed(range(len(caps))):
        over = jnp.int32(0)
        for m in range(matrices):
            over = over + jnp.where(live_ref[m] > pick(caps[v], place_of[m]) * half, 1, 0)
        index = jnp.where(over == 0, v, index)
    index_ref[0] = index


def arrange_kernel(ranked, live_ref, index_ref, slots_ref, out_ref, fetched, placed, in_sem, out_sem):
    matrices, size, width = fetched.shape
    row_index = lax.axis_index("dp") * size + lax.broadcasted_iota(jnp.int32, (size, width), 0)
    place_of = ranks(live_ref, matrices)

    def fetch(m, source):
        return pltpu.make_async_copy(slots_ref.at[source], fetched.at[m], in_sem.at[m])

    def put(m):
        return pltpu.make_async_copy(placed.at[m], out_ref.at[m], out_sem.at[m])

    for m in range(matrices):
        fetch(m, jnp.where(index_ref[0] < ranked, place_of[m], m)).start()

    @pl.loop(0, matrices)
    def _(m):
        fetch(m, m).wait()
        kept = jnp.where(row_index < live_ref[m], fetched[m].astype(jnp.float32), 0.0)
        placed[m] = kept.astype(jnp.bfloat16)
        put(m).start()

    @pl.loop(0, matrices)
    def _(m):
        put(m).wait()


PLANS = (
    ((5, 4, 2, 3, 1, 0, 0, 1), (16, 16, 16, 12, 11, 8, 8, 4), False),
    ((5, 4, 2, 3, 1, 0, 0, 1), (16, 16, 16, 13, 12, 9, 8, 4), False),
    ((5, 4, 3, 2, 0, 1, 2, 1), (16, 16, 16, 15, 12, 12, 8, 4), True),
    ((4, 5, 2, 3, 1, 2, 0, 0), (16, 16, 16, 16, 13, 12, 9, 4), True),
)


def plans_for(n, matrices, size):
    if size % 128 or n % 8 or matrices != n:
        return []
    many = n // 8
    plans = []
    for owners, caps, small_first in PLANS:
        slots = []
        for share in range(8):
            for k in range(many):
                slots.append((share * many + k, owners[share] * many + k, caps[share] * many))
        plans.append(Plan(n, slots, small_first))
    return plans


def solution(mesh):
    n, owners = mesh.shape["dp"], mesh.shape["owner"]
    dma = pltpu.SemaphoreType.DMA

    def dense(rows_live, gradients):
        matrices, size, width = gradients.shape
        hidden = size * n
        strip = max(size, min(128, hidden))
        strips = hidden // strip
        levels = owners.bit_length() - 1
        return pl.pallas_call(
            functools.partial(kernel, n, owners, width * owners),
            out_shape=jax.ShapeDtypeStruct((matrices, size, width), jnp.bfloat16),
            in_specs=[
                pl.BlockSpec(memory_space=pltpu.SMEM),
                pl.BlockSpec(memory_space=pl.ANY),
            ],
            out_specs=pl.BlockSpec(memory_space=pl.ANY),
            scratch_shapes=[
                pltpu.VMEM((n, size, width), jnp.float32),
                pltpu.VMEM((n, size, width), jnp.bfloat16),
                pltpu.VMEM((hidden, width), jnp.bfloat16),
                pltpu.VMEM((hidden, hidden), jnp.float32),
                pltpu.VMEM((hidden, hidden), jnp.bfloat16),
                pltpu.VMEM((hidden, width), jnp.bfloat16),
                pltpu.VMEM((levels, strips, strip, hidden), jnp.bfloat16),
                pltpu.VMEM((levels, strips, strip, hidden), jnp.bfloat16),
                dma((n,)), dma((n,)), dma((n,)),
                dma((levels, strips)), dma((levels, strips)),
                dma((n,)), dma((n,)), dma,
            ],
            compiler_params=pltpu.CompilerParams(
                collective_id=0, has_side_effects=True, vmem_limit_bytes=60 * 2**20
            ),
        )(rows_live, gradients)

    def sparse(plan, number, rows_live, gradients):
        matrices, size, width = gradients.shape
        hidden = size * n
        levels = owners.bit_length() - 1
        most = plan.most
        return pl.pallas_call(
            functools.partial(sparse_kernel, plan, n, owners, width * owners),
            out_shape=jax.ShapeDtypeStruct((matrices, size, width), jnp.bfloat16),
            in_specs=[
                pl.BlockSpec(memory_space=pltpu.SMEM),
                pl.BlockSpec(memory_space=pl.ANY),
            ],
            out_specs=pl.BlockSpec(memory_space=pl.ANY),
            scratch_shapes=[
                pltpu.VMEM((matrices, size, width), jnp.float32),
                pltpu.VMEM((matrices, size, width), jnp.bfloat16),
                pltpu.VMEM((most, hidden, width), jnp.bfloat16),
                pltpu.VMEM((hidden, hidden), jnp.float32),
                pltpu.VMEM((hidden, hidden), jnp.bfloat16),
                pltpu.VMEM((most, hidden, width), jnp.bfloat16),
                pltpu.VMEM((most, n, size, hidden), jnp.bfloat16),
                pltpu.VMEM((most, levels - 1, n, size // 2, hidden), jnp.bfloat16),
                pltpu.VMEM((most, levels, n, size // 2, hidden), jnp.bfloat16),
                pltpu.VMEM((1, size), jnp.float32),
                dma((matrices,)), dma((matrices,)), dma((most, n)),
                dma((most, levels + 1, n)), dma((most, levels + 1, n)),
                dma((most, n)), dma((matrices,)), dma((most,)),
            ],
            compiler_params=pltpu.CompilerParams(
                collective_id=number, has_side_effects=True, vmem_limit_bytes=60 * 2**20
            ),
        )(rows_live, gradients)

    def body(gradients, rows_live):
        matrices, size, _ = gradients.shape
        plans = plans_for(n, matrices, size) if owners > 2 else []
        if not plans:
            return dense(rows_live, gradients)
        smem, anywhere = pl.BlockSpec(memory_space=pltpu.SMEM), pl.BlockSpec(memory_space=pl.ANY)
        index = pl.pallas_call(
            functools.partial(choose_kernel, [p.sorted_caps() for p in plans], size // 2),
            out_shape=jax.ShapeDtypeStruct((1,), jnp.int32),
            in_specs=[smem],
            out_specs=smem,
        )(rows_live)
        branches = [functools.partial(sparse, plan, 1 + v) for v, plan in enumerate(plans)]
        slots = lax.switch(index[0], branches + [dense], rows_live, gradients)
        return pl.pallas_call(
            functools.partial(arrange_kernel, len(plans)),
            out_shape=jax.ShapeDtypeStruct(slots.shape, slots.dtype),
            in_specs=[smem, smem, anywhere],
            out_specs=anywhere,
            scratch_shapes=[
                pltpu.VMEM(slots.shape, slots.dtype),
                pltpu.VMEM(slots.shape, slots.dtype),
                dma((matrices,)), dma((matrices,)),
            ],
        )(rows_live, index, slots)

    return jax.shard_map(
        body,
        mesh=mesh,
        in_specs=(P(None, "dp", "owner"), P()),
        out_specs=P(None, "dp", "owner"),
        check_vma=False,
    )
```

```python
import functools
import math

import jax
import jax.numpy as jnp
from jax import lax
from jax.experimental import pallas as pl
from jax.experimental.pallas import tpu as pltpu
from jax.sharding import PartitionSpec as P

MESH = pl.DeviceIdType.MESH
NT = (((1,), (1,)), ((), ()))
NN = (((1,), (0,)), ((), ()))


def flip(index, bits, count):
    out, bit = 0, 1
    while bit < count:
        out = out + bit * (((index // bit) % 2 + (bits // bit) % 2) % 2)
        bit *= 2
    return out


def kernel(
    n, owners, width_all, live_ref, grad_ref, out_ref,
    stage, send, rows, gram, normed, upd, part, got,
    load_sem, send_sem, recv_sem, psend_sem, precv_sem, usend_sem, urecv_sem, own_sem,
):
    d = lax.axis_index("dp")
    o = lax.axis_index("owner")
    size, width = stage.shape[1], stage.shape[2]
    hidden = rows.shape[0]
    strip = max(size, min(128, hidden))
    strips = hidden // strip
    per = strip // size
    levels = owners.bit_length() - 1

    def far_first(j):
        return 1 + (j + n // 2 - 1) % (n - 1)

    def load(slot):
        return pltpu.make_async_copy(grad_ref.at[flip(d, slot, n)], stage.at[slot], load_sem.at[slot])

    def forward(slot):
        return pltpu.make_async_remote_copy(
            src_ref=send.at[slot],
            dst_ref=rows.at[pl.ds(pl.multiple_of(slot * size, size), size)],
            send_sem=send_sem.at[slot],
            recv_sem=recv_sem.at[slot],
            device_id={"dp": flip(d, slot, n)},
            device_id_type=MESH,
        )

    def back(slot):
        return pltpu.make_async_remote_copy(
            src_ref=upd.at[pl.ds(pl.multiple_of(slot * size, size), size)],
            dst_ref=out_ref.at[d],
            send_sem=usend_sem.at[slot],
            recv_sem=urecv_sem.at[slot],
            device_id={"dp": flip(d, slot, n)},
            device_id_type=MESH,
        )

    def back_arrival(slot):
        return pltpu.make_async_remote_copy(
            src_ref=upd.at[pl.ds(pl.multiple_of(slot * size, size), size)],
            dst_ref=out_ref.at[flip(d, slot, n)],
            send_sem=usend_sem.at[slot],
            recv_sem=urecv_sem.at[slot],
            device_id={"dp": flip(d, slot, n)},
            device_id_type=MESH,
        )

    def share(level, s):
        cols = (s + 1) * strip
        return pltpu.make_async_remote_copy(
            src_ref=part.at[level, s, :, pl.ds(0, cols)],
            dst_ref=got.at[level, s, :, pl.ds(0, cols)],
            send_sem=psend_sem.at[level, s],
            recv_sem=precv_sem.at[level, s],
            device_id={"owner": flip(o, 2**level, owners)},
            device_id_type=MESH,
        )

    @pl.loop(0, n - 1)
    def _(j):
        load(far_first(j)).start()

    load(0).start()

    barrier = pltpu.get_barrier_semaphore()

    @pl.loop(1, n)
    def _(k):
        pl.semaphore_signal(barrier, inc=1, device_id={"dp": flip(d, k, n)}, device_id_type=MESH)

    for level in range(levels):
        pl.semaphore_signal(
            barrier, inc=1, device_id={"owner": flip(o, 2**level, owners)}, device_id_type=MESH
        )
    pl.semaphore_wait(barrier, n - 1 + levels)

    row_index = d * size + lax.broadcasted_iota(jnp.int32, (size, width), 0)

    def narrow(slot):
        load(slot).wait()
        live = live_ref[flip(d, slot, n)]
        return jnp.where(row_index < live, stage[slot], 0.0).astype(jnp.bfloat16)

    @pl.loop(0, n - 1)
    def _(j):
        slot = far_first(j)
        send[slot] = narrow(slot)
        forward(slot).start()

    rows[pl.ds(0, size), :] = narrow(0)

    eye = (
        lax.broadcasted_iota(jnp.int32, (strip, strip), 0)
        == lax.broadcasted_iota(jnp.int32, (strip, strip), 1)
    )
    trace = jnp.zeros((1, 1), jnp.float32)

    def settle(s, trace):
        at = s * strip
        cols = at + strip
        share(levels - 1, s).wait_recv()
        total = (
            part[levels - 1, s, :, 0:cols].astype(jnp.float32)
            + got[levels - 1, s, :, 0:cols].astype(jnp.float32)
        )
        gram[at:cols, 0:cols] = total
        for j in range(s):
            gram[j * strip : (j + 1) * strip, at:cols] = total[:, j * strip : (j + 1) * strip].T
        own = jnp.where(eye, total[:, at:cols], 0.0)
        return trace + jnp.sum(own, keepdims=True)

    for s in range(strips):
        cols = (s + 1) * strip
        if s == 0:
            @pl.loop(1, per)
            def _(k):
                forward(k).wait_recv()
        else:
            @pl.loop(s * per, (s + 1) * per)
            def _(k):
                forward(k).wait_recv()

        part[0, s, :, 0:cols] = lax.dot_general(
            rows[s * strip : cols, :], rows[0:cols, :], NT, preferred_element_type=jnp.float32
        ).astype(jnp.bfloat16)
        share(0, s).start()
        if s > 0:
            trace = settle(s - 1, trace)
        for level in range(1, levels):
            share(level - 1, s).wait_recv()
            part[level, s, :, 0:cols] = (
                part[level - 1, s, :, 0:cols].astype(jnp.float32)
                + got[level - 1, s, :, 0:cols].astype(jnp.float32)
            ).astype(jnp.bfloat16)
            share(level, s).start()
    trace = settle(strips - 1, trace)

    live_count = jnp.full((1, 1), live_ref[d], jnp.int32).astype(jnp.float32)
    scale_sq = 2.0 * trace / live_count
    shrink = 1.0 / scale_sq
    gain = (0.2 * math.sqrt(width_all)) / jnp.sqrt(scale_sq)

    @pl.loop(0, strips)
    def _(s):
        at = pl.ds(pl.multiple_of(s * strip, strip), strip)
        normed[at, :] = (gram[at, :] * shrink).astype(jnp.bfloat16)

    def update(s):
        at = pl.ds(pl.multiple_of(s * strip, strip), strip)
        square = lax.dot_general(normed[at, :], normed[...], NN, preferred_element_type=jnp.float32)
        mix = (2.0315 * square - 4.775 * normed[at, :].astype(jnp.float32)).astype(jnp.bfloat16)
        moved = lax.dot_general(mix, rows[...], NN, preferred_element_type=jnp.float32)
        upd[at, :] = ((3.4445 * rows[at, :].astype(jnp.float32) + moved) * gain).astype(jnp.bfloat16)

    if per == 1:
        @pl.loop(0, n - 1)
        def _(j):
            slot = far_first(j)
            update(slot)
            back(slot).start()

        update(0)
    else:
        @pl.loop(1, strips)
        def _(s):
            update(s)

            @pl.loop(0, per)
            def _(k):
                back(s * per + k).start()

        update(0)

        @pl.loop(1, per)
        def _(k):
            back(k).start()

    own_copy = pltpu.make_async_copy(upd.at[pl.ds(0, size)], out_ref.at[d], own_sem)
    own_copy.start()

    for s in range(strips):
        for level in range(levels):
            share(level, s).wait_send()

    @pl.loop(1, n)
    def _(k):
        forward(k).wait_send()

    @pl.loop(1, n)
    def _(k):
        back(k).wait_send()
        back_arrival(k).wait_recv()

    own_copy.wait()


def pick(values, index):
    out = jnp.int32(values[0]) if isinstance(values[0], int) else values[0]
    for k in range(1, len(values)):
        out = jnp.where(index == k, values[k], out)
    return out


def pick2(rows, row, index):
    return pick([pick(values, index) for values in rows], row)


def ranks(live_ref, matrices):
    lives = [live_ref[m] for m in range(matrices)]
    found = []
    for m in range(matrices):
        ahead = jnp.int32(0)
        for k in range(matrices):
            if k != m:
                before = lives[k] >= lives[m] if k < m else lives[k] > lives[m]
                ahead = ahead + jnp.where(before, 1, 0)
        found.append(ahead)
    return found


class Plan:
    def __init__(self, n, slots, small_first):
        self.ranks = [s[0] for s in slots]
        self.owners = [s[1] for s in slots]
        self.caps = [s[2] for s in slots]

        def late(owner, t):
            far, other = (owner ^ t) >= n // 2, (owner ^ t) % 2
            return (far and other, far, owner ^ t)

        held = [[] for _ in range(n)]
        self.places, self.blocks, self.halves, self.positions = [], [], [], []
        for j in reversed(range(len(slots))) if small_first else range(len(slots)):
            held[self.owners[j]].append(j)
        for j, (owner, cap) in enumerate(zip(self.owners, self.caps)):
            self.places.append(held[owner].index(j))
            blocks = sorted(range(n), key=lambda t: (2 * t >= cap, late(owner, t)))
            self.blocks.append(blocks)
            self.halves.append([min(2, max(0, cap - 2 * t)) for t in blocks])
            self.positions.append([blocks.index(t) for t in range(n)])
        self.orders = [
            sorted(range(len(slots)), key=lambda j: (late(self.owners[j], t)[0], -j)) for t in range(n)
        ]
        self.counts = [len(h) for h in held]
        self.most = max(self.counts)
        self.held = [[h[p] if p < len(h) else 0 for h in held] for p in range(self.most)]
        self.held_caps = [[self.caps[j] for j in row] for row in self.held]

    def sorted_caps(self):
        return [cap for _, cap in sorted(zip(self.ranks, self.caps))]


def sparse_kernel(
    plan, n, owners, width_all, live_ref, grad_ref, out_ref,
    stage, send, rows, gram, normed, upd, part, sums, got, trace,
    load_sem, send_sem, recv_sem, psend_sem, precv_sem, usend_sem, urecv_sem, own_sem,
):
    d = lax.axis_index("dp")
    o = lax.axis_index("owner")
    matrices, size, width = stage.shape
    hidden = rows.shape[1]
    strip, strips, half = size, n, size // 2
    levels = owners.bit_length() - 1

    def strip_at(t):
        return pl.ds(pl.multiple_of(t * size, size), size)

    def load(m):
        return pltpu.make_async_copy(grad_ref.at[m], stage.at[m], load_sem.at[m])

    def part_at(t, halves):
        return pl.ds(pl.multiple_of(t * size, size), halves * half)

    def sent(halves, run):
        pl.when(halves == 2)(functools.partial(run, 2))
        pl.when(halves == 1)(functools.partial(run, 1))

    def forward(j, owner, place, position, halves):
        return pltpu.make_async_remote_copy(
            src_ref=send.at[j, pl.ds(0, halves * half)], dst_ref=rows.at[place, part_at(position, halves)],
            send_sem=send_sem.at[j], recv_sem=recv_sem.at[place, position],
            device_id={"dp": owner}, device_id_type=MESH,
        )

    def back(place, rank, p, t, halves):
        return pltpu.make_async_remote_copy(
            src_ref=upd.at[place, part_at(p, halves)], dst_ref=out_ref.at[rank, pl.ds(0, halves * half)],
            send_sem=usend_sem.at[place, p], recv_sem=urecv_sem.at[rank],
            device_id={"dp": t}, device_id_type=MESH,
        )

    mine = o % 2
    keep = pl.ds(pl.multiple_of(mine * half, half), half)
    give = pl.ds(pl.multiple_of((1 - mine) * half, half), half)

    def owner_copy(src, dst, sent_sem, received_sem, bit):
        return pltpu.make_async_remote_copy(
            src_ref=src, dst_ref=dst, send_sem=sent_sem, recv_sem=received_sem,
            device_id={"owner": flip(o, bit, owners)}, device_id_type=MESH,
        )

    def scatter(place, s):
        cols = pl.ds(0, (s + 1) * strip)
        return owner_copy(
            part.at[place, s, give, cols], got.at[place, 0, s, :, cols],
            psend_sem.at[place, 0, s], precv_sem.at[place, 0, s], 1,
        )

    def share(place, level, s):
        cols = pl.ds(0, (s + 1) * strip)
        return owner_copy(
            sums.at[place, level - 1, s, :, cols], got.at[place, level, s, :, cols],
            psend_sem.at[place, level, s], precv_sem.at[place, level, s], 2**level,
        )

    def gather(place, s):
        at = pl.ds(pl.multiple_of(s * strip + mine * half, half), half)
        here = gram.at[at, pl.ds(0, (s + 1) * strip)]
        return owner_copy(here, here, psend_sem.at[place, levels, s], precv_sem.at[place, levels, s], 1)

    @pl.loop(0, matrices)
    def _(m):
        load(m).start()

    barrier = pltpu.get_barrier_semaphore()

    @pl.loop(1, n)
    def _(k):
        pl.semaphore_signal(barrier, inc=1, device_id={"dp": flip(d, k, n)}, device_id_type=MESH)

    for level in range(levels):
        pl.semaphore_signal(
            barrier, inc=1, device_id={"owner": flip(o, 2**level, owners)}, device_id_type=MESH
        )

    place_of = ranks(live_ref, matrices)
    matrix_of = []
    for j in range(matrices):
        found = jnp.int32(0)
        for m in range(matrices):
            found = found + jnp.where(place_of[m] == plan.ranks[j], m, 0)
        matrix_of.append(found)

    row_index = d * size + lax.broadcasted_iota(jnp.int32, (size, width), 0)

    def narrow(m):
        return jnp.where(row_index < live_ref[m], stage[m], 0.0).astype(jnp.bfloat16)

    count = pick(plan.counts, d)

    def held_slot(place):
        return pick([pick(row, d) for row in plan.held], place)

    def held_cap(place):
        return pick([pick(row, d) for row in plan.held_caps], place)

    pl.semaphore_wait(barrier, n - 1 + levels)

    @pl.loop(0, matrices)
    def _(m):
        load(m).wait()

    @pl.loop(0, matrices)
    def _(i):
        j = pick2(plan.orders, d, i)
        owner, place, m = pick(plan.owners, j), pick(plan.places, j), pick(matrix_of, j)
        position = pick2(plan.positions, j, d)
        halves_sent = pick2(plan.halves, j, position)
        inside = halves_sent > 0

        @pl.when(inside & (owner == d))
        def _():
            rows[place, 0:size, :] = narrow(m)

        @pl.when(inside & (owner != d))
        def _():
            send[j] = narrow(m)
            sent(halves_sent, lambda halves: forward(j, owner, place, position, halves).start())

    eye = (
        lax.broadcasted_iota(jnp.int32, (strip, strip), 0)
        == lax.broadcasted_iota(jnp.int32, (strip, strip), 1)
    )
    column_index = lax.broadcasted_iota(jnp.int32, (strip, hidden), 1)

    @pl.loop(0, count)
    def _(place):
        slot, cap_halves = held_slot(place), held_cap(place)
        rank = pick(plan.ranks, slot)
        cap = (cap_halves + 1) // 2
        live_count = live_ref[pick(matrix_of, slot)]

        @pl.loop(0, n)
        def _(p):
            halves = pick2(plan.halves, slot, p)
            for k in range(2):

                @pl.when(halves <= k)
                def _():
                    at = pl.ds(pl.multiple_of(p * size + k * half, half), half)
                    rows[place, at, :] = jnp.zeros((half, width), jnp.bfloat16)

        @pl.loop(cap, n)
        def _(t):
            normed[strip_at(t), :] = jnp.zeros((strip, hidden), jnp.bfloat16)

        trace[...] = jnp.zeros_like(trace)

        def start(s):
            cols = (s + 1) * strip

            if s > 0:
                sent(
                    pick([halves[s] for halves in plan.halves], slot),
                    lambda halves: forward(0, flip(d, 1, n), place, s, halves).wait_recv(),
                )

            part[place, s, :, 0:cols] = lax.dot_general(
                rows[place, s * strip : cols, :], rows[place, 0:cols, :], NT,
                preferred_element_type=jnp.float32,
            ).astype(jnp.bfloat16)
            scatter(place, s).start()

        def combine(level, s):
            cols = (s + 1) * strip
            if level == 0:
                scatter(place, s).wait_recv()
                own = part[place, s, keep, 0:cols]
            else:
                share(place, level, s).wait_recv()
                own = sums[place, level - 1, s, :, 0:cols]
            total = own.astype(jnp.float32) + got[place, level, s, :, 0:cols].astype(jnp.float32)
            if level < levels - 1:
                sums[place, level, s, :, 0:cols] = total.astype(jnp.bfloat16)
                share(place, level + 1, s).start()
            else:
                gram[pl.ds(pl.multiple_of(s * strip + mine * half, half), half), 0:cols] = total
                gather(place, s).start()

        def settle(s):
            at = s * strip
            cols = at + strip
            gather(place, s).wait_recv()
            for j in range(s):
                gram[j * strip : (j + 1) * strip, at:cols] = gram[at:cols, j * strip : (j + 1) * strip].T
            trace[...] += jnp.sum(jnp.where(eye, gram[at:cols, at:cols], 0.0), axis=0, keepdims=True)

        steps = [start, *[functools.partial(combine, level) for level in range(levels)], settle]
        lags = [0, *range(1, 2 * levels, 2), 2 * levels]
        for at_step in range(strips + max(lags)):
            for run, lag in zip(steps, lags):
                s = at_step - lag
                if 0 <= s < strips:
                    pl.when(s < cap)(functools.partial(run, s))

        whole = jnp.sum(trace[...], keepdims=True)
        scale_sq = 2.0 * whole / jnp.full((1, 1), live_count, jnp.int32).astype(jnp.float32)
        shrink = 1.0 / scale_sq
        gain = (0.2 * math.sqrt(width_all)) / jnp.sqrt(scale_sq)

        for s in range(strips):
            pl.when(s < cap)(gather(place, s).wait_send)

        @pl.loop(0, cap)
        def _(t):
            normed[strip_at(t), :] = jnp.where(
                column_index < cap * strip, gram[strip_at(t), :] * shrink, 0.0
            ).astype(jnp.bfloat16)

        def update(t):
            at = strip_at(t)
            square = lax.dot_general(normed[at, :], normed[...], NN, preferred_element_type=jnp.float32)
            mix = (2.0315 * square - 4.775 * normed[at, :].astype(jnp.float32)).astype(jnp.bfloat16)
            moved = lax.dot_general(mix, rows[place], NN, preferred_element_type=jnp.float32)
            upd[place, at, :] = (
                (3.4445 * rows[place, at, :].astype(jnp.float32) + moved) * gain
            ).astype(jnp.bfloat16)

        @pl.loop(0, cap)
        def _(k):
            p = cap - 1 - k
            t = pick2(plan.blocks, slot, p)
            update(p)

            @pl.when(p > 0)
            def _():
                sent(pick2(plan.halves, slot, p), lambda halves: back(place, rank, p, t, halves).start())

        pltpu.make_async_copy(upd.at[place, pl.ds(0, size)], out_ref.at[rank], own_sem.at[place]).start()

    @pl.loop(0, count)
    def _(place):
        slot, cap_halves = held_slot(place), held_cap(place)
        rank = pick(plan.ranks, slot)
        cap = (cap_halves + 1) // 2
        for s in range(strips):

            @pl.when(s < cap)
            def _():
                scatter(place, s).wait_send()
                for level in range(1, levels):
                    share(place, level, s).wait_send()

        @pl.loop(1, cap)
        def _(p):
            t = pick2(plan.blocks, slot, p)
            sent(pick2(plan.halves, slot, p), lambda halves: back(place, rank, p, t, halves).wait_send())

        pltpu.make_async_copy(upd.at[place, pl.ds(0, size)], out_ref.at[rank], own_sem.at[place]).wait()

    @pl.loop(0, matrices)
    def _(j):
        owner, place, rank = pick(plan.owners, j), pick(plan.places, j), pick(plan.ranks, j)
        position = pick2(plan.positions, j, d)

        @pl.when(owner != d)
        def _():
            def run(halves):
                forward(j, owner, place, position, halves).wait_send()
                back(0, rank, 0, flip(d, 1, n), halves).wait_recv()

            sent(pick2(plan.halves, j, position), run)


def choose_kernel(caps, half, live_ref, index_ref):
    matrices = len(caps[0])
    place_of = ranks(live_ref, matrices)
    index = jnp.int32(len(caps))
    for v in reversed(range(len(caps))):
        over = jnp.int32(0)
        for m in range(matrices):
            over = over + jnp.where(live_ref[m] > pick(caps[v], place_of[m]) * half, 1, 0)
        index = jnp.where(over == 0, v, index)
    index_ref[0] = index


def arrange_kernel(ranked, live_ref, index_ref, slots_ref, out_ref, fetched, placed, blank, in_sem, out_sem):
    matrices, size, width = fetched.shape
    first = lax.axis_index("dp") * size
    row_index = first + lax.broadcasted_iota(jnp.int32, (size, width), 0)
    place_of = ranks(live_ref, matrices)

    def fetch(m, source):
        return pltpu.make_async_copy(slots_ref.at[source], fetched.at[m], in_sem.at[m])

    def put(m, block):
        return pltpu.make_async_copy(block, out_ref.at[m], out_sem.at[m])

    for m in range(matrices):

        @pl.when(live_ref[m] > first)
        def _():
            fetch(m, jnp.where(index_ref[0] < ranked, place_of[m], m)).start()

    blank[...] = jnp.zeros_like(blank)

    @pl.loop(0, matrices)
    def _(m):
        live = live_ref[m]

        @pl.when(live <= first)
        def _():
            put(m, blank).start()

        @pl.when(live > first)
        def _():
            fetch(m, m).wait()

            @pl.when(live >= first + size)
            def _():
                put(m, fetched.at[m]).start()

            @pl.when(live < first + size)
            def _():
                kept = jnp.where(row_index < live, fetched[m].astype(jnp.float32), 0.0)
                placed[m] = kept.astype(jnp.bfloat16)
                put(m, placed.at[m]).start()

    @pl.loop(0, matrices)
    def _(m):
        put(m, blank).wait()


PLANS = (
    ((5, 4, 2, 3, 1, 0, 0, 1), (16, 16, 16, 12, 11, 8, 8, 4), False),
    ((5, 4, 2, 3, 1, 0, 0, 1), (16, 16, 16, 13, 12, 9, 8, 4), False),
    ((5, 4, 3, 2, 0, 1, 2, 1), (16, 16, 16, 15, 12, 12, 8, 4), True),
    ((4, 5, 2, 3, 1, 2, 0, 0), (16, 16, 16, 16, 13, 12, 9, 4), True),
)


def plans_for(n, matrices, size):
    if size % 128 or n % 8 or matrices != n:
        return []
    many = n // 8
    plans = []
    for owners, caps, small_first in PLANS:
        slots = []
        for share in range(8):
            for k in range(many):
                slots.append((share * many + k, owners[share] * many + k, caps[share] * many))
        plans.append(Plan(n, slots, small_first))
    return plans


def solution(mesh):
    n, owners = mesh.shape["dp"], mesh.shape["owner"]
    dma = pltpu.SemaphoreType.DMA

    def dense(rows_live, gradients):
        matrices, size, width = gradients.shape
        hidden = size * n
        strip = max(size, min(128, hidden))
        strips = hidden // strip
        levels = owners.bit_length() - 1
        return pl.pallas_call(
            functools.partial(kernel, n, owners, width * owners),
            out_shape=jax.ShapeDtypeStruct((matrices, size, width), jnp.bfloat16),
            in_specs=[
                pl.BlockSpec(memory_space=pltpu.SMEM),
                pl.BlockSpec(memory_space=pl.ANY),
            ],
            out_specs=pl.BlockSpec(memory_space=pl.ANY),
            scratch_shapes=[
                pltpu.VMEM((n, size, width), jnp.float32),
                pltpu.VMEM((n, size, width), jnp.bfloat16),
                pltpu.VMEM((hidden, width), jnp.bfloat16),
                pltpu.VMEM((hidden, hidden), jnp.float32),
                pltpu.VMEM((hidden, hidden), jnp.bfloat16),
                pltpu.VMEM((hidden, width), jnp.bfloat16),
                pltpu.VMEM((levels, strips, strip, hidden), jnp.bfloat16),
                pltpu.VMEM((levels, strips, strip, hidden), jnp.bfloat16),
                dma((n,)), dma((n,)), dma((n,)),
                dma((levels, strips)), dma((levels, strips)),
                dma((n,)), dma((n,)), dma,
            ],
            compiler_params=pltpu.CompilerParams(
                collective_id=0, has_side_effects=True, vmem_limit_bytes=60 * 2**20
            ),
        )(rows_live, gradients)

    def sparse(plan, number, rows_live, gradients):
        matrices, size, width = gradients.shape
        hidden = size * n
        levels = owners.bit_length() - 1
        most = plan.most
        return pl.pallas_call(
            functools.partial(sparse_kernel, plan, n, owners, width * owners),
            out_shape=jax.ShapeDtypeStruct((matrices, size, width), jnp.bfloat16),
            in_specs=[
                pl.BlockSpec(memory_space=pltpu.SMEM),
                pl.BlockSpec(memory_space=pl.ANY),
            ],
            out_specs=pl.BlockSpec(memory_space=pl.ANY),
            scratch_shapes=[
                pltpu.VMEM((matrices, size, width), jnp.float32),
                pltpu.VMEM((matrices, size, width), jnp.bfloat16),
                pltpu.VMEM((most, hidden, width), jnp.bfloat16),
                pltpu.VMEM((hidden, hidden), jnp.float32),
                pltpu.VMEM((hidden, hidden), jnp.bfloat16),
                pltpu.VMEM((most, hidden, width), jnp.bfloat16),
                pltpu.VMEM((most, n, size, hidden), jnp.bfloat16),
                pltpu.VMEM((most, levels - 1, n, size // 2, hidden), jnp.bfloat16),
                pltpu.VMEM((most, levels, n, size // 2, hidden), jnp.bfloat16),
                pltpu.VMEM((1, size), jnp.float32),
                dma((matrices,)), dma((matrices,)), dma((most, n)),
                dma((most, levels + 1, n)), dma((most, levels + 1, n)),
                dma((most, n)), dma((matrices,)), dma((most,)),
            ],
            compiler_params=pltpu.CompilerParams(
                collective_id=number, has_side_effects=True, vmem_limit_bytes=60 * 2**20
            ),
        )(rows_live, gradients)

    def body(gradients, rows_live):
        matrices, size, _ = gradients.shape
        plans = plans_for(n, matrices, size) if owners > 2 else []
        if not plans:
            return dense(rows_live, gradients)
        smem, anywhere = pl.BlockSpec(memory_space=pltpu.SMEM), pl.BlockSpec(memory_space=pl.ANY)
        index = pl.pallas_call(
            functools.partial(choose_kernel, [p.sorted_caps() for p in plans], size // 2),
            out_shape=jax.ShapeDtypeStruct((1,), jnp.int32),
            in_specs=[smem],
            out_specs=smem,
        )(rows_live)
        branches = [functools.partial(sparse, plan, 1 + v) for v, plan in enumerate(plans)]
        slots = lax.switch(index[0], branches + [dense], rows_live, gradients)
        return pl.pallas_call(
            functools.partial(arrange_kernel, len(plans)),
            out_shape=jax.ShapeDtypeStruct(slots.shape, slots.dtype),
            in_specs=[smem, smem, anywhere],
            out_specs=anywhere,
            scratch_shapes=[
                pltpu.VMEM(slots.shape, slots.dtype),
                pltpu.VMEM(slots.shape, slots.dtype),
                pltpu.VMEM(slots.shape[1:], slots.dtype),
                dma((matrices,)), dma((matrices,)),
            ],
        )(rows_live, index, slots)

    return jax.shard_map(
        body,
        mesh=mesh,
        in_specs=(P(None, "dp", "owner"), P()),
        out_specs=P(None, "dp", "owner"),
        check_vma=False,
    )
```
